32 devices in a mesh: row: 16 (over z, y, core), col: 2 (over x).
Axes of the slice: x: 2, y: 2, z: 4, core: 2. Of those that a mesh axis runs over, the one named last changes fastest.
Arguments:
- pair_act: bfloat16 [192, 192, 128], P('row', 'col'), may hold values from -6 to 6
- tile_mask: int32 [12, 12], replicated, may hold values 0 or 1
- w_left_gate: bfloat16 [128, 128], replicated, may hold values from -0.5 to 0.5
- w_left: bfloat16 [128, 128], replicated, may hold values from -0.5 to 0.5
- w_right_gate: bfloat16 [128, 128], replicated, may hold values from -0.5 to 0.5
- w_right: bfloat16 [128, 128], replicated, may hold values from -0.5 to 0.5
- w_out_gate: bfloat16 [128, 128], replicated, may hold values from -0.5 to 0.5
- w_out: bfloat16 [128, 128], replicated, may hold values from -0.5 to 0.5
Outputs:
- update: bfloat16 [192, 192, 128], P('row', 'col')
The draws below stay inside these ranges and needn't reach their ends.
All inputs are finite; a program needn't handle non-finite values.
Results may differ from the reference program's by a relative error of at most 0.0083.
Values may be sent and summed in bfloat16 or wider, within the bound.
No kernel may reach another device: no remote copies, remote signals or barrier semaphores. Data moves between devices by JAX's collectives and lax.ppermute only.
A program may use at most 64 MiB of HBM per device.

```python
import jax
import jax.numpy as jnp
from jax import lax

CZ = 128
CH = 128
TILES = 12
RES = 192
TILE = 16


def with_ends(result, stream_key, least, largest):
    extent = result.shape
    spot = [jax.random.randint(jax.random.fold_in(stream_key, axis), (), 0, extent[axis]) for axis in range(len(extent))]
    result = result.at[tuple(spot)].set(least)
    longest = extent.index(max(extent))
    spot[longest] = (spot[longest] + 1) % extent[longest]
    return result.at[tuple(spot)].set(largest)


def block_scale(own_key, extent, cuts, low, largest):
    gain, own = 1.0, jax.random.fold_in(own_key, 6)
    for position, shards_of in cuts:
        steps = jnp.exp(jax.random.uniform(jax.random.fold_in(own, position), (shards_of,), jnp.float32, low / len(cuts), largest / len(cuts)))
        gain = gain * jnp.repeat(steps, extent[position] // shards_of).reshape([-1 if axis == position else 1 for axis in range(len(extent))])
    return gain


def normal_values(key, shape, scale, most, cuts=(), kind=jnp.bfloat16):
    entries = scale * jax.random.normal(key, shape, jnp.float32)
    if cuts:
        entries = entries * block_scale(key, shape, cuts, -0.22, 0.18)
    return jnp.clip(entries, -most, most).astype(kind)


def setup_inputs(seed: int = 0) -> dict:
    arg_keys = jax.random.split(jax.random.key(seed), 9)
    return {
        "pair_act": normal_values(arg_keys[0], (RES, RES, CZ), 1.0, 6.0, ((0, 16), (1, 2))),
        "tile_mask": with_ends((jax.random.randint(arg_keys[1], (TILES, TILES), 0, 4) < 3).astype(jnp.int32), jax.random.fold_in(arg_keys[1], 1), 0, 1),
        "w_left_gate": normal_values(arg_keys[2], (CZ, CH), CZ ** -0.5, 0.5),
        "w_left": normal_values(arg_keys[3], (CZ, CH), CZ ** -0.5, 0.5),
        "w_right_gate": normal_values(arg_keys[4], (CZ, CH), CZ ** -0.5, 0.5),
        "w_right": normal_values(arg_keys[5], (CZ, CH), CZ ** -0.5, 0.5),
        "w_out_gate": normal_values(arg_keys[6], (CZ, CZ), CZ ** -0.5, 0.5),
        "w_out": normal_values(arg_keys[7], (CH, CZ), CH ** -0.5, 0.5),
    }


group_width = 8

def norm_last(values):
    mean = lax.optimization_barrier(jnp.mean(values, axis=-1, keepdims=True))
    centred = values - mean
    spread = lax.optimization_barrier(jnp.mean(centred * centred, axis=-1, keepdims=True))
    return centred * lax.rsqrt(spread + 1e-05)

def grouped(weight):
    return weight.reshape(CZ, CH // group_width, group_width).transpose(1, 0, 2)

def reference(pair_act, tile_mask, w_left_gate, w_left, w_right_gate, w_right, w_out_gate, w_out):
    normed = norm_last(pair_act.astype(jnp.float32)).astype(jnp.bfloat16)
    normed_f = lax.optimization_barrier(normed).astype(jnp.float32)
    tile_ids = jnp.arange(RES, dtype=jnp.int32) // TILE
    hot = (tile_ids[:, None] == jnp.arange(TILES, dtype=jnp.int32)[None, :]).astype(jnp.float32)
    pair_mask = jnp.dot(jnp.dot(hot, tile_mask.astype(jnp.float32), preferred_element_type=jnp.float32), hot.T, preferred_element_type=jnp.float32)

    def channel_group(weights):
        left_gate, left_value, right_gate, right_value = weights
        left = jax.nn.sigmoid(jnp.einsum('ikd,de->eik', normed_f, left_gate.astype(jnp.float32)))
        left = (left * jnp.einsum('ikd,de->eik', normed_f, left_value.astype(jnp.float32)) * pair_mask[None]).astype(jnp.bfloat16)
        right = jax.nn.sigmoid(jnp.einsum('jkd,de->ejk', normed_f, right_gate.astype(jnp.float32)))
        right = (right * jnp.einsum('jkd,de->ejk', normed_f, right_value.astype(jnp.float32)) * pair_mask[None]).astype(jnp.bfloat16)
        left_f = lax.optimization_barrier(left).astype(jnp.float32)
        right_f = lax.optimization_barrier(right).astype(jnp.float32)
        return jnp.einsum('cik,cjk->cij', left_f, right_f).astype(jnp.bfloat16)
    triangle = lax.map(channel_group, (grouped(w_left_gate), grouped(w_left), grouped(w_right_gate), grouped(w_right)))
    triangle = triangle.reshape(CH, RES, RES)
    triangle_f = jnp.transpose(lax.optimization_barrier(triangle), (1, 2, 0)).astype(jnp.float32)
    scaled = norm_last(triangle_f).astype(jnp.bfloat16)
    scaled_f = lax.optimization_barrier(scaled).astype(jnp.float32)
    projected = jnp.einsum('ijc,ce->ije', scaled_f, w_out.astype(jnp.float32))
    gate = jax.nn.sigmoid(jnp.einsum('ijd,de->ije', normed_f, w_out_gate.astype(jnp.float32)))
    return (gate * projected).astype(jnp.bfloat16)
```

```python
import functools

import jax
import jax.numpy as jnp
from jax import lax
from jax.experimental import pallas as pl
from jax.experimental.pallas import tpu as pltpu
from jax.sharding import PartitionSpec as P

TILES = 12
LANES = 128
SUBLANES = 8
EPS = 1e-05
F32 = jnp.float32
BF16 = jnp.bfloat16
NT = (((1,), (1,)), ((), ()))
TN = (((0,), (0,)), ((), ()))


def norm_axis(values, axis):
    mean = jnp.mean(values, axis=axis, keepdims=True)
    centred = values - mean
    spread = jnp.mean(centred * centred, axis=axis, keepdims=True)
    return centred * lax.rsqrt(spread + EPS)


def dot(a, b, dims=(((1,), (0,)), ((), ()))):
    return lax.dot_general(a, b, dims, preferred_element_type=F32)


def project_kernel(cols, tile, owned, x_ref, mask_ref, lg_ref, l_ref, rg_ref, r_ref, out_ref):
    pairs, width = x_ref.shape
    channels = l_ref.shape[1]
    row = lax.broadcasted_iota(jnp.int32, (2 * channels, channels), 0)
    channel = lax.broadcasted_iota(jnp.int32, (2 * channels, channels), 1)
    within = row % (2 * owned)
    source = row // (2 * owned) * owned + within % owned
    hit = source == channel
    pick_left = jnp.where(hit & (within < owned), 1.0, 0.0).astype(BF16)
    pick_right = jnp.where(hit & (within >= owned), 1.0, 0.0).astype(BF16)
    gates = (dot(pick_left, lg_ref[...], NT) + dot(pick_right, rg_ref[...], NT)).astype(BF16)
    values = (dot(pick_left, l_ref[...], NT) + dot(pick_right, r_ref[...], NT)).astype(BF16)
    for start in range(0, pairs, LANES):
        normed = norm_axis(x_ref[pl.ds(start, LANES), :].astype(F32), 1).astype(BF16)
        gate = jax.nn.sigmoid(dot(gates, normed, NT))
        value = dot(values, normed, NT)
        kept = mask_ref[:, pl.ds(start, LANES)]
        made = (gate * value * kept).astype(BF16)
        out_ref[:, :, pl.ds(start, LANES)] = made.reshape(out_ref.shape[0], 2 * owned, LANES)


def triangle_kernel(rows, cols, owned, in_ref, out_ref, factors, products):
    blocks, splits = in_ref.shape[0], in_ref.shape[1]
    group = 2 * owned
    for q in range(splits):
        for r in range(blocks):
            flat = in_ref[r, q].astype(F32)
            for i in range(rows):
                at = (r * rows + i) * group
                factors[q, pl.ds(at, group), :] = flat[:, i * cols : (i + 1) * cols]
    residues = blocks * rows
    for c in range(owned):
        left = [factors[q, pl.ds(c, residues, group), :].astype(BF16) for q in range(splits)]
        right = [factors[q, pl.ds(owned + c, residues, group), :].astype(BF16) for q in range(splits)]
        for q in range(splits):
            total = sum(
                dot(left[s], right[s][q * cols : (q + 1) * cols], NT) for s in range(splits)
            )
            products[q, pl.ds(c, residues, owned), :] = total
    for q in range(splits):
        for r in range(blocks):
            pieces = [products[q, pl.ds((r * rows + i) * owned, owned), :] for i in range(rows)]
            out_ref[r, q] = jnp.concatenate(pieces, axis=1).astype(BF16)


def gate_kernel(x_ref, w_ref, out_ref):
    normed = norm_axis(x_ref[...].astype(F32), 1).astype(BF16)
    out_ref[...] = jax.nn.sigmoid(dot(normed, w_ref[...]))


def output_kernel(t_ref, gate_ref, w_ref, out_ref):
    pairs = gate_ref.shape[0]
    for start in range(0, pairs, LANES):
        scaled = norm_axis(t_ref[:, pl.ds(start, LANES)].astype(F32), 0).astype(BF16)
        projected = dot(scaled, w_ref[...], TN)
        here = pl.ds(start, LANES)
        out_ref[here, :] = (gate_ref[here, :] * projected).astype(BF16)


def call(body, out, scratch=(), flops=0, **params):
    return pl.pallas_call(
        body,
        out_shape=out,
        scratch_shapes=list(scratch),
        cost_estimate=pl.CostEstimate(flops=flops, bytes_accessed=flops // 100, transcendentals=0),
        compiler_params=pltpu.CompilerParams(**params),
    )


def mask_of(tile_mask, rows, cols):
    tile = rows * lax.axis_size("row") // TILES
    tile_range = lax.iota(jnp.int32, TILES)
    row_ids = (lax.axis_index("row") * rows + lax.iota(jnp.int32, rows)) // tile
    col_ids = (lax.axis_index("col") * cols + lax.iota(jnp.int32, cols)) // tile
    row_hot = (row_ids[:, None] == tile_range[None, :]).astype(F32)
    col_hot = (col_ids[:, None] == tile_range[None, :]).astype(F32)
    some = dot(row_hot, tile_mask.astype(F32))
    return dot(some, col_hot.T)


def by_channels(pair_act, tile_mask, w_left_gate, w_left, w_right_gate, w_right, w_out_gate, w_out):
    rows, cols, width = pair_act.shape
    blocks, splits = lax.axis_size("row"), lax.axis_size("col")
    devices = blocks * splits
    channels = w_left.shape[1]
    owned = channels // devices
    pairs = rows * cols
    tile = rows * blocks // TILES
    flat = pair_act.reshape(pairs, width)
    pair_mask = mask_of(tile_mask, rows, cols).reshape(1, pairs)
    factors = call(
        functools.partial(project_kernel, cols, tile, owned),
        jax.ShapeDtypeStruct((devices, 2 * owned, pairs), BF16),
        flops=8 * pairs * width * channels,
    )(flat, pair_mask, w_left_gate, w_left, w_right_gate, w_right)
    factors = lax.all_to_all(factors, ("row", "col"), 0, 0, tiled=True)
    gate = call(
        gate_kernel, jax.ShapeDtypeStruct((pairs, width), F32), flops=2 * pairs * width * width
    )(flat, w_out_gate)
    residues = rows * blocks
    triangle = call(
        functools.partial(triangle_kernel, rows, cols, owned),
        jax.ShapeDtypeStruct((blocks, splits, owned, pairs), BF16),
        scratch=(
            pltpu.VMEM((splits, residues * 2 * owned, cols), F32),
            pltpu.VMEM((splits, residues * owned, cols), F32),
        ),
        flops=2 * owned * residues**3,
    )(factors.reshape(blocks, splits, 2 * owned, pairs))
    owned_pairs = lax.all_to_all(
        triangle.reshape(devices, owned, pairs), ("row", "col"), 0, 0, tiled=True
    )
    out = call(
        output_kernel,
        jax.ShapeDtypeStruct((pairs, width), BF16),
        flops=2 * pairs * width * channels,
    )(owned_pairs.reshape(channels, pairs), gate, w_out)
    return out.reshape(rows, cols, width)


def by_rows(pair_act, tile_mask, w_left_gate, w_left, w_right_gate, w_right, w_out_gate, w_out):
    rows, cols, width = pair_act.shape
    normed = norm_axis(pair_act.astype(F32), 2).astype(BF16)
    pair_mask = mask_of(tile_mask, rows, cols)

    def project(weight):
        return jnp.einsum("ijd,de->eij", normed, weight, preferred_element_type=F32)

    left = (jax.nn.sigmoid(project(w_left_gate)) * project(w_left) * pair_mask[None]).astype(BF16)
    right = (jax.nn.sigmoid(project(w_right_gate)) * project(w_right) * pair_mask[None]).astype(
        BF16
    )
    left_rows, right_rows = (
        lax.all_to_all(left, "row", split_axis=0, concat_axis=1, tiled=True),
        lax.all_to_all(right, "row", split_axis=0, concat_axis=1, tiled=True),
    )
    right_block = lax.all_to_all(right_rows, "col", split_axis=1, concat_axis=2, tiled=True)
    triangle = jnp.einsum(
        "cik,cjk->jci",
        lax.all_gather(left_rows, "col", axis=2, tiled=True),
        right_block,
        preferred_element_type=F32,
    )
    triangle = triangle.astype(BF16)
    owned = lax.all_to_all(triangle, "row", split_axis=2, concat_axis=1, tiled=True)
    scaled = norm_axis(owned.astype(F32), 1).astype(BF16)
    projected = jnp.einsum("jci,ce->ije", scaled, w_out, preferred_element_type=F32)
    gate = jax.nn.sigmoid(jnp.einsum("ijd,de->ije", normed, w_out_gate, preferred_element_type=F32))
    return (gate * projected).astype(BF16)


def local(pair_act, tile_mask, w_left_gate, *weights):
    devices = lax.axis_size("row") * lax.axis_size("col")
    rows, cols, width = pair_act.shape
    channels = w_left_gate.shape[1]
    whole = channels % devices == 0 and 2 * channels // devices % SUBLANES == 0
    aligned = rows * cols % LANES == 0 and cols % SUBLANES == 0 and cols <= LANES
    form = by_channels if whole and aligned else by_rows
    return form(pair_act, tile_mask, w_left_gate, *weights)


def solution(mesh):
    return jax.shard_map(
        local,
        mesh=mesh,
        in_specs=(P("row", "col", None), P(), P(), P(), P(), P(), P(), P()),
        out_specs=P("row", "col", None),
        check_vma=False,
    )
```

```python
import functools

import jax
import jax.numpy as jnp
from jax import lax
from jax.experimental import pallas as pl
from jax.experimental.pallas import tpu as pltpu
from jax.sharding import PartitionSpec as P

TILES = 12
LANES = 128
SUBLANES = 8
EPS = 1e-05
GRANT = 16 * 2**20
WIDE = 60 * 2**20
F32 = jnp.float32
BF16 = jnp.bfloat16
NT = (((1,), (1,)), ((), ()))
TN = (((0,), (0,)), ((), ()))


def norm_axis(values, axis):
    mean = jnp.mean(values, axis=axis, keepdims=True)
    centred = values - mean
    spread = jnp.mean(centred * centred, axis=axis, keepdims=True)
    return centred * lax.rsqrt(spread + EPS)


def dot(a, b, dims=(((1,), (0,)), ((), ()))):
    return lax.dot_general(a, b, dims, preferred_element_type=F32)


def lane_mask(cols, tile, pairs, rows, tiles):
    kinds = tiles.shape[0]
    place = lax.broadcasted_iota(jnp.int32, (kinds, pairs), 1).astype(F32) + 0.5
    kind = lax.broadcasted_iota(jnp.int32, (kinds, pairs), 0).astype(F32)
    row = jnp.floor(place * (1.0 / cols))
    col = place - row * cols
    first_row = (lax.axis_index("row") * rows).astype(F32)
    first_col = (lax.axis_index("col") * cols).astype(F32)
    row_kind = jnp.floor((row + first_row + 0.5) * (1.0 / tile))
    col_kind = jnp.floor((col + first_col) * (1.0 / tile))
    row_hot = jnp.where(row_kind == kind, 1.0, 0.0)
    col_hot = jnp.where(col_kind == kind, 1.0, 0.0).astype(BF16)
    return jnp.sum(row_hot * dot(tiles.astype(F32).astype(BF16), col_hot), axis=0, keepdims=True)


def project_kernel(rows, tile, owned, *refs):
    far, (out_far, gate_far), near, (out_ref, gate_ref) = refs[:7], refs[7:9], refs[9:16], refs[16:18]
    in_sems, out_sems = refs[18:]
    copies = [pltpu.make_async_copy(a, b, in_sems.at[n]) for n, (a, b) in enumerate(zip(far, near))]
    for copy in copies:
        copy.start()
    x_ref, tiles_ref, lg_ref, l_ref, rg_ref, r_ref, og_ref = near
    pairs, width = x_ref.shape
    channels = l_ref.shape[1]
    row = lax.broadcasted_iota(jnp.int32, (2 * channels, channels), 0)
    channel = lax.broadcasted_iota(jnp.int32, (2 * channels, channels), 1)
    within = row % (2 * owned)
    source = row // (2 * owned) * owned + within % owned
    hit = source == channel
    pick_left = jnp.where(hit & (within < owned), 1.0, 0.0).astype(BF16)
    pick_right = jnp.where(hit & (within >= owned), 1.0, 0.0).astype(BF16)
    for copy in copies:
        copy.wait()
    gates = (dot(pick_left, lg_ref[...], NT) + dot(pick_right, rg_ref[...], NT)).astype(BF16)
    values = (dot(pick_left, l_ref[...], NT) + dot(pick_right, r_ref[...], NT)).astype(BF16)
    mask = lane_mask(pairs // rows, tile, pairs, rows, tiles_ref[...])
    sent = []
    for n, start in enumerate(range(0, pairs, LANES)):
        here = pl.ds(start, LANES)
        normed = norm_axis(x_ref[here, :].astype(F32), 1).astype(BF16)
        gate = jax.nn.sigmoid(dot(gates, normed, NT))
        value = dot(values, normed, NT)
        made = (gate * value * mask[:, start : start + LANES]).astype(BF16)
        out_ref[:, :, here] = made.reshape(out_ref.shape[0], 2 * owned, LANES)
        gate_ref[here, :] = jax.nn.sigmoid(dot(normed, og_ref[...]))
        out_slice, gate_slice = (slice(None), slice(None), here), (here, slice(None))
        for m, (near_ref, far_ref, part) in enumerate(
            ((out_ref, out_far, out_slice), (gate_ref, gate_far, gate_slice))
        ):
            sent.append(
                pltpu.make_async_copy(near_ref.at[part], far_ref.at[part], out_sems.at[m, n])
            )
            sent[-1].start()
    for copy in sent:
        copy.wait()


def triangle_kernel(rows, cols, owned, in_ref, out_ref, factors, products):
    blocks, splits = in_ref.shape[0], in_ref.shape[1]
    group = 2 * owned
    for q in range(splits):
        for r in range(blocks):
            flat = in_ref[r, q].astype(F32)
            for i in range(rows):
                at = (r * rows + i) * group
                factors[q, pl.ds(at, group), :] = flat[:, i * cols : (i + 1) * cols]
    residues = blocks * rows
    for c in range(owned):
        left = [factors[q, pl.ds(c, residues, group), :].astype(BF16) for q in range(splits)]
        right = [factors[q, pl.ds(owned + c, residues, group), :].astype(BF16) for q in range(splits)]
        for q in range(splits):
            total = sum(
                dot(left[s], right[s][q * cols : (q + 1) * cols], NT) for s in range(splits)
            )
            products[q, pl.ds(c, residues, owned), :] = total
    for q in range(splits):
        for r in range(blocks):
            pieces = [products[q, pl.ds((r * rows + i) * owned, owned), :] for i in range(rows)]
            out_ref[r, q] = jnp.concatenate(pieces, axis=1).astype(BF16)


def output_kernel(t_ref, gate_ref, w_ref, out_ref):
    pairs = gate_ref.shape[0]
    channels = w_ref.shape[0]
    for start in range(0, pairs, LANES):
        triangle = t_ref[:, :, pl.ds(start, LANES)].reshape(channels, LANES).astype(F32)
        scaled = norm_axis(triangle, 0).astype(BF16)
        projected = dot(scaled, w_ref[...], TN)
        here = pl.ds(start, LANES)
        out_ref[here, :] = (gate_ref[here, :] * projected).astype(BF16)


def call(body, out, operands, scratch=(), flops=0, space=pltpu.VMEM, grant=GRANT):
    return pl.pallas_call(
        body,
        out_shape=out,
        in_specs=[pl.BlockSpec(memory_space=space)] * len(operands),
        out_specs=jax.tree.map(lambda _: pl.BlockSpec(memory_space=space), out),
        scratch_shapes=list(scratch),
        cost_estimate=pl.CostEstimate(flops=flops, bytes_accessed=flops // 100, transcendentals=0),
        compiler_params=pltpu.CompilerParams(vmem_limit_bytes=grant),
    )(*operands)


def mask_of(tile_mask, rows, cols):
    tile = rows * lax.axis_size("row") // TILES
    tile_range = lax.iota(jnp.int32, TILES)
    row_ids = (lax.axis_index("row") * rows + lax.iota(jnp.int32, rows)) // tile
    col_ids = (lax.axis_index("col") * cols + lax.iota(jnp.int32, cols)) // tile
    row_hot = (row_ids[:, None] == tile_range[None, :]).astype(F32)
    col_hot = (col_ids[:, None] == tile_range[None, :]).astype(F32)
    some = dot(row_hot, tile_mask.astype(F32))
    return dot(some, col_hot.T)


def by_channels(pair_act, tile_mask, w_left_gate, w_left, w_right_gate, w_right, w_out_gate, w_out):
    rows, cols, width = pair_act.shape
    blocks, splits = lax.axis_size("row"), lax.axis_size("col")
    devices = blocks * splits
    channels = w_left.shape[1]
    owned = channels // devices
    pairs = rows * cols
    tile = rows * blocks // TILES
    flat = pair_act.reshape(pairs, width)
    operands = (flat, tile_mask, w_left_gate, w_left, w_right_gate, w_right, w_out_gate)
    made = (
        jax.ShapeDtypeStruct((devices, 2 * owned, pairs), BF16),
        jax.ShapeDtypeStruct((pairs, width), F32),
    )
    factors, gate = call(
        functools.partial(project_kernel, rows, tile, owned),
        made,
        operands,
        scratch=[pltpu.VMEM(a.shape, a.dtype) for a in operands + made]
        + [pltpu.SemaphoreType.DMA((n,)) for n in (len(operands),)]
        + [pltpu.SemaphoreType.DMA((len(made), pairs // LANES))],
        flops=10 * pairs * width * channels,
        space=pltpu.HBM,
        grant=WIDE,
    )
    factors = lax.all_to_all(factors, ("row", "col"), 0, 0, tiled=True)
    residues = rows * blocks
    triangle = call(
        functools.partial(triangle_kernel, rows, cols, owned),
        jax.ShapeDtypeStruct((blocks, splits, owned, pairs), BF16),
        (factors.reshape(blocks, splits, 2 * owned, pairs),),
        scratch=(
            pltpu.VMEM((splits, residues * 2 * owned, cols), F32),
            pltpu.VMEM((splits, residues * owned, cols), F32),
        ),
        flops=2 * owned * residues**3,
    )
    owned_pairs = lax.all_to_all(
        triangle.reshape(devices, owned, pairs), ("row", "col"), 0, 0, tiled=True
    )
    out = call(
        output_kernel,
        jax.ShapeDtypeStruct((pairs, width), BF16),
        (owned_pairs, gate, w_out),
        flops=2 * pairs * width * channels,
    )
    return out.reshape(rows, cols, width)


def by_rows(pair_act, tile_mask, w_left_gate, w_left, w_right_gate, w_right, w_out_gate, w_out):
    rows, cols, width = pair_act.shape
    normed = norm_axis(pair_act.astype(F32), 2).astype(BF16)
    pair_mask = mask_of(tile_mask, rows, cols)

    def project(weight):
        return jnp.einsum("ijd,de->eij", normed, weight, preferred_element_type=F32)

    left = (jax.nn.sigmoid(project(w_left_gate)) * project(w_left) * pair_mask[None]).astype(BF16)
    right = (jax.nn.sigmoid(project(w_right_gate)) * project(w_right) * pair_mask[None]).astype(
        BF16
    )
    left_rows, right_rows = (
        lax.all_to_all(left, "row", split_axis=0, concat_axis=1, tiled=True),
        lax.all_to_all(right, "row", split_axis=0, concat_axis=1, tiled=True),
    )
    right_block = lax.all_to_all(right_rows, "col", split_axis=1, concat_axis=2, tiled=True)
    triangle = jnp.einsum(
        "cik,cjk->jci",
        lax.all_gather(left_rows, "col", axis=2, tiled=True),
        right_block,
        preferred_element_type=F32,
    )
    triangle = triangle.astype(BF16)
    owned = lax.all_to_all(triangle, "row", split_axis=2, concat_axis=1, tiled=True)
    scaled = norm_axis(owned.astype(F32), 1).astype(BF16)
    projected = jnp.einsum("jci,ce->ije", scaled, w_out, preferred_element_type=F32)
    gate = jax.nn.sigmoid(jnp.einsum("ijd,de->ije", normed, w_out_gate, preferred_element_type=F32))
    return (gate * projected).astype(BF16)


def local(pair_act, tile_mask, w_left_gate, *weights):
    devices = lax.axis_size("row") * lax.axis_size("col")
    rows, cols, width = pair_act.shape
    channels = w_left_gate.shape[1]
    whole = channels % devices == 0 and 2 * channels // devices % SUBLANES == 0
    aligned = rows * cols % LANES == 0 and cols % SUBLANES == 0 and cols <= LANES
    form = by_channels if whole and aligned else by_rows
    return form(pair_act, tile_mask, w_left_gate, *weights)


def solution(mesh):
    return jax.shard_map(
        local,
        mesh=mesh,
        in_specs=(P("row", "col", None), P(), P(), P(), P(), P(), P(), P()),
        out_specs=P("row", "col", None),
        check_vma=False,
    )
```

```python
import functools

import jax
import jax.numpy as jnp
from jax import lax
from jax.experimental import pallas as pl
from jax.experimental.pallas import tpu as pltpu
from jax.sharding import PartitionSpec as P

TILES = 12
LANES = 128
SUBLANES = 8
EPS = 1e-05
GRANT = 16 * 2**20
F32 = jnp.float32
BF16 = jnp.bfloat16
NT = (((1,), (1,)), ((), ()))
TN = (((0,), (0,)), ((), ()))


def norm_axis(values, axis):
    mean = jnp.mean(values, axis=axis, keepdims=True)
    centred = values - mean
    spread = jnp.mean(centred * centred, axis=axis, keepdims=True)
    return centred * lax.rsqrt(spread + EPS)


def dot(a, b, dims=(((1,), (0,)), ((), ()))):
    return lax.dot_general(a, b, dims, preferred_element_type=F32)


def lane_mask(cols, tile, pairs, rows, tiles):
    kinds = tiles.shape[0]
    place = lax.broadcasted_iota(jnp.int32, (kinds, pairs), 1).astype(F32) + 0.5
    kind = lax.broadcasted_iota(jnp.int32, (kinds, pairs), 0).astype(F32)
    row = jnp.floor(place * (1.0 / cols))
    col = place - row * cols
    first_row = (lax.axis_index("row") * rows).astype(F32)
    first_col = (lax.axis_index("col") * cols).astype(F32)
    row_kind = jnp.floor((row + first_row + 0.5) * (1.0 / tile))
    col_kind = jnp.floor((col + first_col) * (1.0 / tile))
    row_hot = jnp.where(row_kind == kind, 1.0, 0.0)
    col_hot = jnp.where(col_kind == kind, 1.0, 0.0).astype(BF16)
    return jnp.sum(row_hot * dot(tiles.astype(F32).astype(BF16), col_hot), axis=0, keepdims=True)


def project_kernel(rows, tile, owned, *refs):
    far, (out_ref, gate_ref), near, sems = refs[:7], refs[7:9], refs[9:16], refs[16]
    copies = [pltpu.make_async_copy(a, b, sems.at[n]) for n, (a, b) in enumerate(zip(far, near))]
    for copy in copies:
        copy.start()
    x_ref, tiles_ref, lg_ref, l_ref, rg_ref, r_ref, og_ref = near
    pairs, width = x_ref.shape
    channels = l_ref.shape[1]
    row = lax.broadcasted_iota(jnp.int32, (2 * channels, channels), 0)
    channel = lax.broadcasted_iota(jnp.int32, (2 * channels, channels), 1)
    within = row % (2 * owned)
    source = row // (2 * owned) * owned + within % owned
    hit = source == channel
    pick_left = jnp.where(hit & (within < owned), 1.0, 0.0).astype(BF16)
    pick_right = jnp.where(hit & (within >= owned), 1.0, 0.0).astype(BF16)
    for copy in copies:
        copy.wait()
    gates = (dot(pick_left, lg_ref[...], NT) + dot(pick_right, rg_ref[...], NT)).astype(BF16)
    values = (dot(pick_left, l_ref[...], NT) + dot(pick_right, r_ref[...], NT)).astype(BF16)
    mask = lane_mask(pairs // rows, tile, pairs, rows, tiles_ref[...])
    for start in range(0, pairs, LANES):
        here = pl.ds(start, LANES)
        normed = norm_axis(x_ref[here, :].astype(F32), 1).astype(BF16)
        gate = jax.nn.sigmoid(dot(gates, normed, NT))
        value = dot(values, normed, NT)
        made = (gate * value * mask[:, start : start + LANES]).astype(BF16)
        out_ref[:, :, here] = made.reshape(out_ref.shape[0], 2 * owned, LANES)
        gate_ref[here, :] = jax.nn.sigmoid(dot(normed, og_ref[...]))


def triangle_kernel(rows, cols, owned, in_ref, out_ref, factors, products):
    blocks, splits = in_ref.shape[0], in_ref.shape[1]
    group = 2 * owned
    for q in range(splits):
        for r in range(blocks):
            flat = in_ref[r, q].astype(F32)
            for i in range(rows):
                at = (r * rows + i) * group
                factors[q, pl.ds(at, group), :] = flat[:, i * cols : (i + 1) * cols]
    residues = blocks * rows
    for c in range(owned):
        left = [factors[q, pl.ds(c, residues, group), :].astype(BF16) for q in range(splits)]
        right = [factors[q, pl.ds(owned + c, residues, group), :].astype(BF16) for q in range(splits)]
        for q in range(splits):
            total = sum(
                dot(left[s], right[s][q * cols : (q + 1) * cols], NT) for s in range(splits)
            )
            products[q, pl.ds(c, residues, owned), :] = total
    for q in range(splits):
        for r in range(blocks):
            pieces = [products[q, pl.ds((r * rows + i) * owned, owned), :] for i in range(rows)]
            out_ref[r, q] = jnp.concatenate(pieces, axis=1).astype(BF16)


def output_kernel(t_ref, gate_ref, w_ref, out_ref):
    pairs = gate_ref.shape[0]
    channels = w_ref.shape[0]
    for start in range(0, pairs, LANES):
        triangle = t_ref[:, :, pl.ds(start, LANES)].reshape(channels, LANES).astype(F32)
        scaled = norm_axis(triangle, 0).astype(BF16)
        projected = dot(scaled, w_ref[...], TN)
        here = pl.ds(start, LANES)
        out_ref[here, :] = (gate_ref[here, :] * projected).astype(BF16)


def call(body, out, operands, scratch=(), flops=0, space=pltpu.VMEM):
    return pl.pallas_call(
        body,
        out_shape=out,
        in_specs=[pl.BlockSpec(memory_space=space)] * len(operands),
        out_specs=jax.tree.map(lambda _: pl.BlockSpec(memory_space=pltpu.VMEM), out),
        scratch_shapes=list(scratch),
        cost_estimate=pl.CostEstimate(flops=flops, bytes_accessed=flops // 100, transcendentals=0),
        compiler_params=pltpu.CompilerParams(vmem_limit_bytes=GRANT),
    )(*[pltpu.with_memory_space_constraint(a, space) for a in operands])


def mask_of(tile_mask, rows, cols):
    tile = rows * lax.axis_size("row") // TILES
    tile_range = lax.iota(jnp.int32, TILES)
    row_ids = (lax.axis_index("row") * rows + lax.iota(jnp.int32, rows)) // tile
    col_ids = (lax.axis_index("col") * cols + lax.iota(jnp.int32, cols)) // tile
    row_hot = (row_ids[:, None] == tile_range[None, :]).astype(F32)
    col_hot = (col_ids[:, None] == tile_range[None, :]).astype(F32)
    some = dot(row_hot, tile_mask.astype(F32))
    return dot(some, col_hot.T)


def by_channels(pair_act, tile_mask, w_left_gate, w_left, w_right_gate, w_right, w_out_gate, w_out):
    rows, cols, width = pair_act.shape
    blocks, splits = lax.axis_size("row"), lax.axis_size("col")
    devices = blocks * splits
    channels = w_left.shape[1]
    owned = channels // devices
    pairs = rows * cols
    tile = rows * blocks // TILES
    flat = pair_act.reshape(pairs, width)
    operands = (flat, tile_mask, w_left_gate, w_left, w_right_gate, w_right, w_out_gate)
    factors, gate = call(
        functools.partial(project_kernel, rows, tile, owned),
        (pltpu.VMEM((devices, 2 * owned, pairs), BF16), pltpu.VMEM((pairs, width), F32)),
        operands,
        scratch=[pltpu.VMEM(a.shape, a.dtype) for a in operands]
        + [pltpu.SemaphoreType.DMA((len(operands),))],
        flops=10 * pairs * width * channels,
        space=pltpu.HBM,
    )
    factors = lax.all_to_all(factors, ("row", "col"), 0, 0, tiled=True)
    residues = rows * blocks
    triangle = call(
        functools.partial(triangle_kernel, rows, cols, owned),
        pltpu.VMEM((blocks, splits, owned, pairs), BF16),
        (factors.reshape(blocks, splits, 2 * owned, pairs),),
        scratch=(
            pltpu.VMEM((splits, residues * 2 * owned, cols), F32),
            pltpu.VMEM((splits, residues * owned, cols), F32),
        ),
        flops=2 * owned * residues**3,
    )
    owned_pairs = lax.all_to_all(
        triangle.reshape(devices, owned, pairs), ("row", "col"), 0, 0, tiled=True
    )
    out = call(
        output_kernel,
        jax.ShapeDtypeStruct((pairs, width), BF16),
        (owned_pairs, gate, w_out),
        flops=2 * pairs * width * channels,
    )
    return out.reshape(rows, cols, width)


def by_rows(pair_act, tile_mask, w_left_gate, w_left, w_right_gate, w_right, w_out_gate, w_out):
    rows, cols, width = pair_act.shape
    normed = norm_axis(pair_act.astype(F32), 2).astype(BF16)
    pair_mask = mask_of(tile_mask, rows, cols)

    def project(weight):
        return jnp.einsum("ijd,de->eij", normed, weight, preferred_element_type=F32)

    left = (jax.nn.sigmoid(project(w_left_gate)) * project(w_left) * pair_mask[None]).astype(BF16)
    right = (jax.nn.sigmoid(project(w_right_gate)) * project(w_right) * pair_mask[None]).astype(
        BF16
    )
    left_rows, right_rows = (
        lax.all_to_all(left, "row", split_axis=0, concat_axis=1, tiled=True),
        lax.all_to_all(right, "row", split_axis=0, concat_axis=1, tiled=True),
    )
    right_block = lax.all_to_all(right_rows, "col", split_axis=1, concat_axis=2, tiled=True)
    triangle = jnp.einsum(
        "cik,cjk->jci",
        lax.all_gather(left_rows, "col", axis=2, tiled=True),
        right_block,
        preferred_element_type=F32,
    )
    triangle = triangle.astype(BF16)
    owned = lax.all_to_all(triangle, "row", split_axis=2, concat_axis=1, tiled=True)
    scaled = norm_axis(owned.astype(F32), 1).astype(BF16)
    projected = jnp.einsum("jci,ce->ije", scaled, w_out, preferred_element_type=F32)
    gate = jax.nn.sigmoid(jnp.einsum("ijd,de->ije", normed, w_out_gate, preferred_element_type=F32))
    return (gate * projected).astype(BF16)


def local(pair_act, tile_mask, w_left_gate, *weights):
    devices = lax.axis_size("row") * lax.axis_size("col")
    rows, cols, width = pair_act.shape
    channels = w_left_gate.shape[1]
    whole = channels % devices == 0 and 2 * channels // devices % SUBLANES == 0
    aligned = rows * cols % LANES == 0 and cols % SUBLANES == 0 and cols <= LANES
    form = by_channels if whole and aligned else by_rows
    return form(pair_act, tile_mask, w_left_gate, *weights)


def solution(mesh):
    return jax.shard_map(
        local,
        mesh=mesh,
        in_specs=(P("row", "col", None), P(), P(), P(), P(), P(), P(), P()),
        out_specs=P("row", "col", None),
        check_vma=False,
    )
```

```python
import functools

import jax
import jax.numpy as jnp
from jax import lax
from jax.experimental import pallas as pl
from jax.experimental.pallas import tpu as pltpu
from jax.sharding import PartitionSpec as P

TILES = 12
LANES = 128
SUBLANES = 8
EPS = 1e-05
GRANT = 16 * 2**20
F32 = jnp.float32
BF16 = jnp.bfloat16
NT = (((1,), (1,)), ((), ()))
TN = (((0,), (0,)), ((), ()))


def norm_axis(values, axis):
    mean = jnp.mean(values, axis=axis, keepdims=True)
    centred = values - mean
    spread = jnp.mean(centred * centred, axis=axis, keepdims=True)
    return centred * lax.rsqrt(spread + EPS)


def dot(a, b, dims=(((1,), (0,)), ((), ()))):
    return lax.dot_general(a, b, dims, preferred_element_type=F32)


def lane_mask(cols, tile, pairs, rows, tiles):
    kinds = tiles.shape[0]
    place = lax.broadcasted_iota(jnp.int32, (kinds, pairs), 1).astype(F32) + 0.5
    kind = lax.broadcasted_iota(jnp.int32, (kinds, pairs), 0).astype(F32)
    row = jnp.floor(place * (1.0 / cols))
    col = place - row * cols
    first_row = (lax.axis_index("row") * rows).astype(F32)
    first_col = (lax.axis_index("col") * cols).astype(F32)
    row_kind = jnp.floor((row + first_row + 0.5) * (1.0 / tile))
    col_kind = jnp.floor((col + first_col) * (1.0 / tile))
    row_hot = jnp.where(row_kind == kind, 1.0, 0.0)
    col_hot = jnp.where(col_kind == kind, 1.0, 0.0).astype(BF16)
    return jnp.sum(row_hot * dot(tiles.astype(F32).astype(BF16), col_hot), axis=0, keepdims=True)


def project_kernel(rows, tile, owned, *refs):
    far, (out_ref, gate_ref), near, sems = refs[:7], refs[7:9], refs[9:16], refs[16]
    copies = [pltpu.make_async_copy(a, b, sems.at[n]) for n, (a, b) in enumerate(zip(far, near))]
    for copy in copies:
        copy.start()
    x_ref, tiles_ref, lg_ref, l_ref, rg_ref, r_ref, og_ref = near
    pairs, width = x_ref.shape
    channels = l_ref.shape[1]
    row = lax.broadcasted_iota(jnp.int32, (2 * channels, channels), 0)
    channel = lax.broadcasted_iota(jnp.int32, (2 * channels, channels), 1)
    within = row % (2 * owned)
    source = row // (2 * owned) * owned + within % owned
    hit = source == channel
    pick_left = jnp.where(hit & (within < owned), 1.0, 0.0).astype(BF16)
    pick_right = jnp.where(hit & (within >= owned), 1.0, 0.0).astype(BF16)
    for copy in copies:
        copy.wait()
    gates = (dot(pick_left, lg_ref[...], NT) + dot(pick_right, rg_ref[...], NT)).astype(BF16)
    values = (dot(pick_left, l_ref[...], NT) + dot(pick_right, r_ref[...], NT)).astype(BF16)
    mask = lane_mask(pairs // rows, tile, pairs, rows, tiles_ref[...])
    for start in range(0, pairs, LANES):
        here = pl.ds(start, LANES)
        normed = norm_axis(x_ref[here, :].astype(F32), 1).astype(BF16)
        gate = jax.nn.sigmoid(dot(gates, normed, NT))
        value = dot(values, normed, NT)
        made = (gate * value * mask[:, start : start + LANES]).astype(BF16)
        out_ref[:, :, here] = made.reshape(out_ref.shape[0], 2 * owned, LANES)
        gate_ref[here, :] = jax.nn.sigmoid(dot(normed, og_ref[...]))


def triangle_kernel(rows, cols, owned, in_ref, out_ref, factors, products):
    splits, blocks = in_ref.shape[0], in_ref.shape[1]
    group = 2 * owned
    for q in range(splits):
        for r in range(blocks):
            flat = in_ref[q, r].astype(F32)
            for i in range(rows):
                at = (r * rows + i) * group
                factors[q, pl.ds(at, group), :] = flat[:, i * cols : (i + 1) * cols]
    residues = blocks * rows
    for c in range(owned):
        left = [factors[q, pl.ds(c, residues, group), :].astype(BF16) for q in range(splits)]
        right = [factors[q, pl.ds(owned + c, residues, group), :].astype(BF16) for q in range(splits)]
        for q in range(splits):
            total = sum(
                dot(left[s], right[s][q * cols : (q + 1) * cols], NT) for s in range(splits)
            )
            products[q, pl.ds(c, residues, owned), :] = total
    for q in range(splits):
        for r in range(blocks):
            pieces = [products[q, pl.ds((r * rows + i) * owned, owned), :] for i in range(rows)]
            out_ref[q, r] = jnp.concatenate(pieces, axis=1).astype(BF16)


def output_kernel(t_ref, gate_ref, w_ref, out_ref):
    pairs = gate_ref.shape[0]
    channels = w_ref.shape[0]
    for start in range(0, pairs, LANES):
        triangle = t_ref[:, :, pl.ds(start, LANES)].reshape(channels, LANES).astype(F32)
        scaled = norm_axis(triangle, 0).astype(BF16)
        projected = dot(scaled, w_ref[...], TN)
        here = pl.ds(start, LANES)
        out_ref[here, :] = (gate_ref[here, :] * projected).astype(BF16)


def call(body, out, operands, scratch=(), flops=0, space=pltpu.VMEM):
    return pl.pallas_call(
        body,
        out_shape=out,
        in_specs=[pl.BlockSpec(memory_space=space)] * len(operands),
        out_specs=jax.tree.map(lambda _: pl.BlockSpec(memory_space=pltpu.VMEM), out),
        scratch_shapes=list(scratch),
        cost_estimate=pl.CostEstimate(flops=flops, bytes_accessed=flops // 100, transcendentals=0),
        compiler_params=pltpu.CompilerParams(vmem_limit_bytes=GRANT),
    )(*[pltpu.with_memory_space_constraint(a, space) for a in operands])


def mask_of(tile_mask, rows, cols):
    tile = rows * lax.axis_size("row") // TILES
    tile_range = lax.iota(jnp.int32, TILES)
    row_ids = (lax.axis_index("row") * rows + lax.iota(jnp.int32, rows)) // tile
    col_ids = (lax.axis_index("col") * cols + lax.iota(jnp.int32, cols)) // tile
    row_hot = (row_ids[:, None] == tile_range[None, :]).astype(F32)
    col_hot = (col_ids[:, None] == tile_range[None, :]).astype(F32)
    some = dot(row_hot, tile_mask.astype(F32))
    return dot(some, col_hot.T)


def by_channels(pair_act, tile_mask, w_left_gate, w_left, w_right_gate, w_right, w_out_gate, w_out):
    rows, cols, width = pair_act.shape
    blocks, splits = lax.axis_size("row"), lax.axis_size("col")
    devices = blocks * splits
    channels = w_left.shape[1]
    owned = channels // devices
    pairs = rows * cols
    tile = rows * blocks // TILES
    flat = pair_act.reshape(pairs, width)
    operands = (flat, tile_mask, w_left_gate, w_left, w_right_gate, w_right, w_out_gate)
    factors, gate = call(
        functools.partial(project_kernel, rows, tile, owned),
        (pltpu.VMEM((devices, 2 * owned, pairs), BF16), pltpu.VMEM((pairs, width), F32)),
        operands,
        scratch=[pltpu.VMEM(a.shape, a.dtype) for a in operands]
        + [pltpu.SemaphoreType.DMA((len(operands),))],
        flops=10 * pairs * width * channels,
        space=pltpu.HBM,
    )
    factors = lax.all_to_all(factors, ("col", "row"), 0, 0, tiled=True)
    residues = rows * blocks
    triangle = call(
        functools.partial(triangle_kernel, rows, cols, owned),
        pltpu.VMEM((splits, blocks, owned, pairs), BF16),
        (factors.reshape(splits, blocks, 2 * owned, pairs),),
        scratch=(
            pltpu.VMEM((splits, residues * 2 * owned, cols), F32),
            pltpu.VMEM((splits, residues * owned, cols), F32),
        ),
        flops=2 * owned * residues**3,
    )
    owned_pairs = lax.all_to_all(
        triangle.reshape(devices, owned, pairs), ("col", "row"), 0, 0, tiled=True
    )
    out = call(
        output_kernel,
        jax.ShapeDtypeStruct((pairs, width), BF16),
        (owned_pairs, gate, w_out),
        flops=2 * pairs * width * channels,
    )
    return out.reshape(rows, cols, width)


def by_rows(pair_act, tile_mask, w_left_gate, w_left, w_right_gate, w_right, w_out_gate, w_out):
    rows, cols, width = pair_act.shape
    normed = norm_axis(pair_act.astype(F32), 2).astype(BF16)
    pair_mask = mask_of(tile_mask, rows, cols)

    def project(weight):
        return jnp.einsum("ijd,de->eij", normed, weight, preferred_element_type=F32)

    left = (jax.nn.sigmoid(project(w_left_gate)) * project(w_left) * pair_mask[None]).astype(BF16)
    right = (jax.nn.sigmoid(project(w_right_gate)) * project(w_right) * pair_mask[None]).astype(
        BF16
    )
    left_rows, right_rows = (
        lax.all_to_all(left, "row", split_axis=0, concat_axis=1, tiled=True),
        lax.all_to_all(right, "row", split_axis=0, concat_axis=1, tiled=True),
    )
    right_block = lax.all_to_all(right_rows, "col", split_axis=1, concat_axis=2, tiled=True)
    triangle = jnp.einsum(
        "cik,cjk->jci",
        lax.all_gather(left_rows, "col", axis=2, tiled=True),
        right_block,
        preferred_element_type=F32,
    )
    triangle = triangle.astype(BF16)
    owned = lax.all_to_all(triangle, "row", split_axis=2, concat_axis=1, tiled=True)
    scaled = norm_axis(owned.astype(F32), 1).astype(BF16)
    projected = jnp.einsum("jci,ce->ije", scaled, w_out, preferred_element_type=F32)
    gate = jax.nn.sigmoid(jnp.einsum("ijd,de->ije", normed, w_out_gate, preferred_element_type=F32))
    return (gate * projected).astype(BF16)


def local(pair_act, tile_mask, w_left_gate, *weights):
    devices = lax.axis_size("row") * lax.axis_size("col")
    rows, cols, width = pair_act.shape
    channels = w_left_gate.shape[1]
    whole = channels % devices == 0 and 2 * channels // devices % SUBLANES == 0
    aligned = rows * cols % LANES == 0 and cols % SUBLANES == 0 and cols <= LANES
    form = by_channels if whole and aligned else by_rows
    return form(pair_act, tile_mask, w_left_gate, *weights)


def solution(mesh):
    return jax.shard_map(
        local,
        mesh=mesh,
        in_specs=(P("row", "col", None), P(), P(), P(), P(), P(), P(), P()),
        out_specs=P("row", "col", None),
        check_vma=False,
    )
```

```python
import functools

import jax
import jax.numpy as jnp
from jax import lax
from jax.experimental import pallas as pl
from jax.experimental.pallas import tpu as pltpu
from jax.sharding import PartitionSpec as P

TILES = 12
LANES = 128
WIDE = 256
OWIDE = 256
SUBLANES = 8
EPS = 1e-05
GRANT = 16 * 2**20
F32 = jnp.float32
BF16 = jnp.bfloat16
NT = (((1,), (1,)), ((), ()))
TN = (((0,), (0,)), ((), ()))


def norm_axis(values, axis):
    mean = jnp.mean(values, axis=axis, keepdims=True)
    centred = values - mean
    spread = jnp.mean(centred * centred, axis=axis, keepdims=True)
    return centred * lax.rsqrt(spread + EPS)


def dot(a, b, dims=(((1,), (0,)), ((), ()))):
    return lax.dot_general(a, b, dims, preferred_element_type=F32)


def lane_mask(cols, tile, pairs, rows, tiles):
    kinds = tiles.shape[0]
    place = lax.broadcasted_iota(jnp.int32, (kinds, pairs), 1).astype(F32) + 0.5
    kind = lax.broadcasted_iota(jnp.int32, (kinds, pairs), 0).astype(F32)
    row = jnp.floor(place * (1.0 / cols))
    col = place - row * cols
    first_row = (lax.axis_index("row") * rows).astype(F32)
    first_col = (lax.axis_index("col") * cols).astype(F32)
    row_kind = jnp.floor((row + first_row + 0.5) * (1.0 / tile))
    col_kind = jnp.floor((col + first_col) * (1.0 / tile))
    row_hot = jnp.where(row_kind == kind, 1.0, 0.0)
    col_hot = jnp.where(col_kind == kind, 1.0, 0.0).astype(BF16)
    return jnp.sum(row_hot * dot(tiles.astype(F32).astype(BF16), col_hot), axis=0, keepdims=True)


def project_kernel(rows, tile, owned, *refs):
    far, (out_ref, gate_ref), near, sems = refs[:7], refs[7:9], refs[9:16], refs[16]
    copies = [pltpu.make_async_copy(a, b, sems.at[n]) for n, (a, b) in enumerate(zip(far, near))]
    for copy in copies:
        copy.start()
    x_ref, tiles_ref, lg_ref, l_ref, rg_ref, r_ref, og_ref = near
    pairs, width = x_ref.shape
    channels = l_ref.shape[1]
    row = lax.broadcasted_iota(jnp.int32, (2 * channels, channels), 0)
    channel = lax.broadcasted_iota(jnp.int32, (2 * channels, channels), 1)
    within = row % (2 * owned)
    source = row // (2 * owned) * owned + within % owned
    hit = source == channel
    pick_left = jnp.where(hit & (within < owned), 1.0, 0.0).astype(BF16)
    pick_right = jnp.where(hit & (within >= owned), 1.0, 0.0).astype(BF16)
    for copy in copies:
        copy.wait()
    gates = (dot(pick_left, lg_ref[...], NT) + dot(pick_right, rg_ref[...], NT)).astype(BF16)
    values = (dot(pick_left, l_ref[...], NT) + dot(pick_right, r_ref[...], NT)).astype(BF16)
    mask = lane_mask(pairs // rows, tile, pairs, rows, tiles_ref[...]).astype(BF16)
    for start in range(0, pairs, WIDE):
        wide = min(WIDE, pairs - start)
        here = pl.ds(start, wide)
        normed = norm_axis(x_ref[here, :].astype(F32), 1).astype(BF16)
        gate = jax.nn.sigmoid(dot(gates, normed, NT))
        value = dot(values, normed, NT)
        made = (gate * value).astype(BF16) * mask[:, start : start + wide]
        out_ref[:, :, here] = made.reshape(out_ref.shape[0], 2 * owned, wide)
        gate_ref[here, :] = jax.nn.sigmoid(dot(normed, og_ref[...]))


def triangle_kernel(rows, cols, owned, in_ref, out_ref, factors, products):
    splits, blocks = in_ref.shape[0], in_ref.shape[1]
    group = 2 * owned
    for q in range(splits):
        for r in range(blocks):
            flat = in_ref[q, r].astype(F32)
            for i in range(rows):
                at = (r * rows + i) * group
                factors[q, pl.ds(at, group), :] = flat[:, i * cols : (i + 1) * cols]
    residues = blocks * rows
    gap = LANES - cols
    for c in range(owned):
        left = [factors[q, pl.ds(c, residues, group), :].astype(BF16) for q in range(splits)]
        right = [factors[q, pl.ds(owned + c, residues, group), :].astype(BF16) for q in range(splits)]
        empty = jnp.zeros((gap, cols), BF16)
        spread = [
            jnp.concatenate(
                [p for q in range(splits) for p in (r[q * cols : (q + 1) * cols], empty)], axis=0
            )
            for r in right
        ]
        none = jnp.zeros((residues, gap), BF16)
        lefts = jnp.concatenate([p for l in left for p in (l, none)], axis=1)
        none = jnp.zeros((splits * LANES, gap), BF16)
        rights = jnp.concatenate([p for r in spread for p in (r, none)], axis=1)
        total = dot(lefts, rights, NT)
        for q in range(splits):
            products[q, pl.ds(c, residues, owned), :] = total[:, q * LANES : q * LANES + cols]
    for q in range(splits):
        for r in range(blocks):
            pieces = [products[q, pl.ds((r * rows + i) * owned, owned), :] for i in range(rows)]
            out_ref[q, r] = jnp.concatenate(pieces, axis=1).astype(BF16)


def output_kernel(t_ref, gate_ref, w_ref, out_ref):
    pairs = gate_ref.shape[0]
    channels = w_ref.shape[0]
    for start in range(0, pairs, OWIDE):
        wide = min(OWIDE, pairs - start)
        triangle = t_ref[:, :, pl.ds(start, wide)].reshape(channels, wide).astype(F32)
        scaled = norm_axis(triangle, 0).astype(BF16)
        projected = dot(scaled, w_ref[...], TN)
        here = pl.ds(start, wide)
        out_ref[here, :] = (gate_ref[here, :] * projected).astype(BF16)


def call(body, out, operands, scratch=(), flops=0, space=pltpu.VMEM):
    return pl.pallas_call(
        body,
        out_shape=out,
        in_specs=[pl.BlockSpec(memory_space=space)] * len(operands),
        out_specs=jax.tree.map(lambda _: pl.BlockSpec(memory_space=pltpu.VMEM), out),
        scratch_shapes=list(scratch),
        cost_estimate=pl.CostEstimate(flops=flops, bytes_accessed=flops // 100, transcendentals=0),
        compiler_params=pltpu.CompilerParams(vmem_limit_bytes=GRANT),
    )(*[pltpu.with_memory_space_constraint(a, space) for a in operands])


def mask_of(tile_mask, rows, cols):
    tile = rows * lax.axis_size("row") // TILES
    tile_range = lax.iota(jnp.int32, TILES)
    row_ids = (lax.axis_index("row") * rows + lax.iota(jnp.int32, rows)) // tile
    col_ids = (lax.axis_index("col") * cols + lax.iota(jnp.int32, cols)) // tile
    row_hot = (row_ids[:, None] == tile_range[None, :]).astype(F32)
    col_hot = (col_ids[:, None] == tile_range[None, :]).astype(F32)
    some = dot(row_hot, tile_mask.astype(F32))
    return dot(some, col_hot.T)


def by_channels(pair_act, tile_mask, w_left_gate, w_left, w_right_gate, w_right, w_out_gate, w_out):
    rows, cols, width = pair_act.shape
    blocks, splits = lax.axis_size("row"), lax.axis_size("col")
    devices = blocks * splits
    channels = w_left.shape[1]
    owned = channels // devices
    pairs = rows * cols
    tile = rows * blocks // TILES
    flat = pair_act.reshape(pairs, width)
    operands = (flat, tile_mask, w_left_gate, w_left, w_right_gate, w_right, w_out_gate)
    factors, gate = call(
        functools.partial(project_kernel, rows, tile, owned),
        (pltpu.VMEM((devices, 2 * owned, pairs), BF16), pltpu.VMEM((pairs, width), F32)),
        operands,
        scratch=[pltpu.VMEM(a.shape, a.dtype) for a in operands]
        + [pltpu.SemaphoreType.DMA((len(operands),))],
        flops=10 * pairs * width * channels,
        space=pltpu.HBM,
    )
    factors = lax.all_to_all(factors, ("col", "row"), 0, 0, tiled=True)
    residues = rows * blocks
    triangle = call(
        functools.partial(triangle_kernel, rows, cols, owned),
        pltpu.VMEM((splits, blocks, owned, pairs), BF16),
        (factors.reshape(splits, blocks, 2 * owned, pairs),),
        scratch=(
            pltpu.VMEM((splits, residues * 2 * owned, cols), F32),
            pltpu.VMEM((splits, residues * owned, cols), F32),
        ),
        flops=2 * owned * residues**3,
    )
    owned_pairs = lax.all_to_all(
        triangle.reshape(devices, owned, pairs), ("col", "row"), 0, 0, tiled=True
    )
    out = call(
        output_kernel,
        jax.ShapeDtypeStruct((pairs, width), BF16),
        (owned_pairs, gate, w_out),
        flops=2 * pairs * width * channels,
    )
    return out.reshape(rows, cols, width)


def by_rows(pair_act, tile_mask, w_left_gate, w_left, w_right_gate, w_right, w_out_gate, w_out):
    rows, cols, width = pair_act.shape
    normed = norm_axis(pair_act.astype(F32), 2).astype(BF16)
    pair_mask = mask_of(tile_mask, rows, cols)

    def project(weight):
        return jnp.einsum("ijd,de->eij", normed, weight, preferred_element_type=F32)

    left = (jax.nn.sigmoid(project(w_left_gate)) * project(w_left) * pair_mask[None]).astype(BF16)
    right = (jax.nn.sigmoid(project(w_right_gate)) * project(w_right) * pair_mask[None]).astype(
        BF16
    )
    left_rows, right_rows = (
        lax.all_to_all(left, "row", split_axis=0, concat_axis=1, tiled=True),
        lax.all_to_all(right, "row", split_axis=0, concat_axis=1, tiled=True),
    )
    right_block = lax.all_to_all(right_rows, "col", split_axis=1, concat_axis=2, tiled=True)
    triangle = jnp.einsum(
        "cik,cjk->jci",
        lax.all_gather(left_rows, "col", axis=2, tiled=True),
        right_block,
        preferred_element_type=F32,
    )
    triangle = triangle.astype(BF16)
    owned = lax.all_to_all(triangle, "row", split_axis=2, concat_axis=1, tiled=True)
    scaled = norm_axis(owned.astype(F32), 1).astype(BF16)
    projected = jnp.einsum("jci,ce->ije", scaled, w_out, preferred_element_type=F32)
    gate = jax.nn.sigmoid(jnp.einsum("ijd,de->ije", normed, w_out_gate, preferred_element_type=F32))
    return (gate * projected).astype(BF16)


def local(pair_act, tile_mask, w_left_gate, *weights):
    devices = lax.axis_size("row") * lax.axis_size("col")
    rows, cols, width = pair_act.shape
    channels = w_left_gate.shape[1]
    whole = channels % devices == 0 and 2 * channels // devices % SUBLANES == 0
    aligned = rows * cols % LANES == 0 and cols % SUBLANES == 0 and cols <= LANES
    form = by_channels if whole and aligned else by_rows
    return form(pair_act, tile_mask, w_left_gate, *weights)


def solution(mesh):
    return jax.shard_map(
        local,
        mesh=mesh,
        in_specs=(P("row", "col", None), P(), P(), P(), P(), P(), P(), P()),
        out_specs=P("row", "col", None),
        check_vma=False,
    )
```

```python
import functools

import jax
import jax.numpy as jnp
from jax import lax
from jax.experimental import pallas as pl
from jax.experimental.pallas import tpu as pltpu
from jax.sharding import PartitionSpec as P


TILES = 12
LANES = 128
WIDE = 256
OWIDE = 256
SUBLANES = 8
EPS = 1e-05
GRANT = 16 * 2**20
F32 = jnp.float32
BF16 = jnp.bfloat16
NT = (((1,), (1,)), ((), ()))
TN = (((0,), (0,)), ((), ()))


def norm_axis(values, axis):
    mean = jnp.mean(values, axis=axis, keepdims=True)
    centred = values - mean
    spread = jnp.mean(centred * centred, axis=axis, keepdims=True)
    return centred * lax.rsqrt(spread + EPS)


def dot(a, b, dims=(((1,), (0,)), ((), ()))):
    return lax.dot_general(a, b, dims, preferred_element_type=F32)


def lane_mask(cols, tile, pairs, rows, tiles):
    kinds = tiles.shape[0]
    place = lax.broadcasted_iota(jnp.int32, (kinds, pairs), 1).astype(F32) + 0.5
    kind = lax.broadcasted_iota(jnp.int32, (kinds, pairs), 0).astype(F32)
    row = jnp.floor(place * (1.0 / cols))
    col = place - row * cols
    first_row = (lax.axis_index("row") * rows).astype(F32)
    first_col = (lax.axis_index("col") * cols).astype(F32)
    row_kind = jnp.floor((row + first_row + 0.5) * (1.0 / tile))
    col_kind = jnp.floor((col + first_col) * (1.0 / tile))
    row_hot = jnp.where(row_kind == kind, 1.0, 0.0)
    col_hot = jnp.where(col_kind == kind, 1.0, 0.0).astype(BF16)
    return jnp.sum(row_hot * dot(tiles.astype(F32).astype(BF16), col_hot), axis=0, keepdims=True)


def project_kernel(rows, tile, owned, *refs):
    far, (out_ref, gate_ref), near, sems = refs[:7], refs[7:9], refs[9:16], refs[16]
    copies = [pltpu.make_async_copy(a, b, sems.at[n]) for n, (a, b) in enumerate(zip(far, near))]
    for copy in copies:
        copy.start()
    x_ref, tiles_ref, lg_ref, l_ref, rg_ref, r_ref, og_ref = near
    pairs, _ = x_ref.shape
    channels = l_ref.shape[1]
    row = lax.broadcasted_iota(jnp.int32, (2 * channels, channels), 0)
    channel = lax.broadcasted_iota(jnp.int32, (2 * channels, channels), 1)
    within = row % (2 * owned)
    source = row // (2 * owned) * owned + within % owned
    hit = source == channel
    pick_left = jnp.where(hit & (within < owned), 1.0, 0.0).astype(BF16)
    pick_right = jnp.where(hit & (within >= owned), 1.0, 0.0).astype(BF16)
    for copy in copies:
        copy.wait()
    gates = (dot(pick_left, lg_ref[...], NT) + dot(pick_right, rg_ref[...], NT)).astype(BF16)
    values = (dot(pick_left, l_ref[...], NT) + dot(pick_right, r_ref[...], NT)).astype(BF16)
    mask = lane_mask(pairs // rows, tile, pairs, rows, tiles_ref[...]).astype(BF16)
    for start in range(0, pairs, WIDE):
        wide = min(WIDE, pairs - start)
        here = pl.ds(start, wide)
        normed = norm_axis(x_ref[here, :].astype(F32), 1).astype(BF16)
        gate = jax.nn.sigmoid(dot(gates, normed, NT))
        value = dot(values, normed, NT)
        made = (gate * value).astype(BF16) * mask[:, start : start + wide]
        out_ref[:, :, here] = made.reshape(out_ref.shape[0], 2 * owned, wide)
        gate_ref[here, :] = jax.nn.sigmoid(dot(normed, og_ref[...]))


def triangle_kernel(rows, cols, owned, in_ref, out_ref, factors, products):
    splits, blocks = in_ref.shape[0], in_ref.shape[1]
    group = 2 * owned
    for q in range(splits):
        for r in range(blocks):
            flat = in_ref[q, r].astype(F32)
            for i in range(rows):
                at = (r * rows + i) * group
                factors[q, pl.ds(at, group), :] = flat[:, i * cols : (i + 1) * cols]
    residues = blocks * rows
    gap = LANES - cols
    for c in range(owned):
        left = [factors[q, pl.ds(c, residues, group), :].astype(BF16) for q in range(splits)]
        right = [factors[q, pl.ds(owned + c, residues, group), :].astype(BF16) for q in range(splits)]
        empty = jnp.zeros((gap, cols), BF16)
        spread = [
            jnp.concatenate(
                [p for q in range(splits) for p in (r[q * cols : (q + 1) * cols], empty)], axis=0
            )
            for r in right
        ]
        none = jnp.zeros((residues, gap), BF16)
        lefts = jnp.concatenate([p for l in left for p in (l, none)], axis=1)
        none = jnp.zeros((splits * LANES, gap), BF16)
        rights = jnp.concatenate([p for r in spread for p in (r, none)], axis=1)
        total = dot(lefts, rights, NT)
        for q in range(splits):
            products[q, pl.ds(c, residues, owned), :] = total[:, q * LANES : q * LANES + cols]
    for q in range(splits):
        for r in range(blocks):
            pieces = [products[q, pl.ds((r * rows + i) * owned, owned), :] for i in range(rows)]
            out_ref[q, r] = jnp.concatenate(pieces, axis=1).astype(BF16)


def output_kernel(t_ref, gate_ref, w_ref, out_ref):
    pairs = gate_ref.shape[0]
    channels = w_ref.shape[0]
    for start in range(0, pairs, OWIDE):
        wide = min(OWIDE, pairs - start)
        triangle = t_ref[:, :, pl.ds(start, wide)].reshape(channels, wide).astype(F32)
        scaled = norm_axis(triangle, 0).astype(BF16)
        projected = dot(scaled, w_ref[...], TN)
        here = pl.ds(start, wide)
        out_ref[here, :] = (gate_ref[here, :] * projected).astype(BF16)


def space_of(out):
    return getattr(out, "memory_space", pltpu.VMEM)


def call(body, out, operands, scratch=(), flops=0, space=pltpu.VMEM):
    return pl.pallas_call(
        body,
        out_shape=out,
        in_specs=[pl.BlockSpec(memory_space=space)] * len(operands),
        out_specs=jax.tree.map(lambda o: pl.BlockSpec(memory_space=space_of(o)), out),
        scratch_shapes=list(scratch),
        cost_estimate=pl.CostEstimate(flops=flops, bytes_accessed=flops // 100, transcendentals=0),
        compiler_params=pltpu.CompilerParams(vmem_limit_bytes=GRANT),
    )(*[pltpu.with_memory_space_constraint(a, space) for a in operands])


def mask_of(tile_mask, rows, cols):
    tile = rows * lax.axis_size("row") // TILES
    tile_range = lax.iota(jnp.int32, TILES)
    row_ids = (lax.axis_index("row") * rows + lax.iota(jnp.int32, rows)) // tile
    col_ids = (lax.axis_index("col") * cols + lax.iota(jnp.int32, cols)) // tile
    row_hot = (row_ids[:, None] == tile_range[None, :]).astype(F32)
    col_hot = (col_ids[:, None] == tile_range[None, :]).astype(F32)
    some = dot(row_hot, tile_mask.astype(F32))
    return dot(some, col_hot.T)


def by_channels(pair_act, tile_mask, w_left_gate, w_left, w_right_gate, w_right, w_out_gate, w_out):
    rows, cols, width = pair_act.shape
    blocks, splits = lax.axis_size("row"), lax.axis_size("col")
    devices = blocks * splits
    channels = w_left.shape[1]
    owned = channels // devices
    pairs = rows * cols
    tile = rows * blocks // TILES
    flat = pair_act.reshape(pairs, width)
    operands = (flat, tile_mask, w_left_gate, w_left, w_right_gate, w_right, w_out_gate)
    factors, gate = call(
        functools.partial(project_kernel, rows, tile, owned),
        (pltpu.VMEM((devices, 2 * owned, pairs), BF16), pltpu.VMEM((pairs, width), F32)),
        operands,
        scratch=[pltpu.VMEM(a.shape, a.dtype) for a in operands]
        + [pltpu.SemaphoreType.DMA((len(operands),))],
        flops=10 * pairs * width * channels,
        space=pltpu.HBM,
    )
    factors = lax.all_to_all(factors, ("col", "row"), 0, 0, tiled=True)
    residues = rows * blocks
    triangle = call(
        functools.partial(triangle_kernel, rows, cols, owned),
        pltpu.VMEM((splits, blocks, owned, pairs), BF16),
        (factors.reshape(splits, blocks, 2 * owned, pairs),),
        scratch=(
            pltpu.VMEM((splits, residues * 2 * owned, cols), F32),
            pltpu.VMEM((splits, residues * owned, cols), F32),
        ),
        flops=2 * owned * residues**3,
    )
    owned_pairs = lax.all_to_all(
        triangle.reshape(devices, owned, pairs), ("col", "row"), 0, 0, tiled=True
    )
    out = call(
        output_kernel,
        jax.ShapeDtypeStruct((pairs, width), BF16),
        (owned_pairs, gate, w_out),
        flops=2 * pairs * width * channels,
    )
    return out.reshape(rows, cols, width)


def halves_project_kernel(rows, tile, owned, *refs):
    far, (left_ref, right_far, gate_ref), near = refs[:7], refs[7:10], refs[10:17]
    right_ref, normed_ref, sems, right_sems = refs[17:]
    copies = [pltpu.make_async_copy(a, b, sems.at[n]) for n, (a, b) in enumerate(zip(far, near))]
    for copy in copies:
        copy.start()
    x_ref, tiles_ref, lg_ref, l_ref, rg_ref, r_ref, og_ref = near
    pairs, _ = x_ref.shape
    channels = l_ref.shape[1]
    members = channels // owned
    row = lax.broadcasted_iota(jnp.int32, (channels, channels), 0)
    channel = lax.broadcasted_iota(jnp.int32, (channels, channels), 1)
    owner = (row // owned) ^ member_number(members)
    pick_left = jnp.where(owner * owned + row % owned == channel, 1.0, 0.0).astype(BF16)
    pick_right = jnp.where(row == channel, 1.0, 0.0).astype(BF16)
    for copy in copies:
        copy.wait()
    mask = lane_mask(pairs // rows, tile, pairs, rows, tiles_ref[...]).astype(BF16)
    _, halves, _ = right_far.shape[:3]

    def factor(pick, gate_w, value_w, target):
        gates = dot(pick, gate_w[...], NT).astype(BF16)
        values = dot(pick, value_w[...], NT).astype(BF16)

        def make(normed, start, wide):
            gate = jax.nn.sigmoid(dot(gates, normed, NT))
            made = (gate * dot(values, normed, NT)).astype(BF16) * mask[:, start : start + wide]
            target[..., pl.ds(start, wide)] = made.reshape(*target.shape[:-1], wide)

        return make

    make_right = factor(pick_right, rg_ref, r_ref, right_ref)
    make_left = factor(pick_left, lg_ref, l_ref, left_ref)
    strips = [(start, min(WIDE, pairs - start)) for start in range(0, pairs, WIDE)]
    for start, wide in strips:
        here = pl.ds(start, wide)
        normed = norm_axis(x_ref[here, :].astype(F32), 1).astype(BF16)
        normed_ref[here, :] = normed
        make_right(normed, start, wide)
    sent = [
        pltpu.make_async_copy(right_ref, right_far.at[:, half], right_sems.at[half])
        for half in range(halves)
    ]
    for copy in sent:
        copy.start()
    for start, wide in strips:
        here = pl.ds(start, wide)
        normed = normed_ref[here, :]
        make_left(normed, start, wide)
        gate_ref[here, :] = jax.nn.sigmoid(dot(normed, og_ref[...]))
    for copy in sent:
        copy.wait()


def member_number(members):
    near_rows = members // lax.axis_size("col")
    return lax.axis_index("col") * near_rows + lax.axis_index("row") % near_rows


def halves_triangle_kernel(rows, cols, members, steps, *refs):
    left_refs, (right_ref, out_ref, lefts, rights, products) = refs[: len(steps)], refs[len(steps) :]
    splits, blocks, owned = right_ref.shape[:3]
    near_rows = members // splits
    for q in range(splits):
        for r in range(blocks):
            flat = right_ref[q, r].astype(F32)
            for i in range(rows):
                at = (r * rows + i) * owned
                rights[q, pl.ds(at, owned), :] = flat[:, i * cols : (i + 1) * cols]
    me = member_number(members)
    for left_ref, distances in zip(left_refs, steps):
        for n, distance in enumerate(distances):
            source = me ^ distance
            q, r = source // near_rows, source % near_rows
            flat = left_ref[n].astype(F32)
            for i in range(rows):
                at = pl.multiple_of((r * rows + i) * owned, owned)
                lefts[q, pl.ds(at, owned), :] = flat[:, i * cols : (i + 1) * cols]
    residues, half = blocks * rows, near_rows * rows
    gap = LANES - cols
    for c in range(owned):
        left = [lefts[q, pl.ds(c, half, owned), :].astype(BF16) for q in range(splits)]
        right = [rights[q, pl.ds(c, residues, owned), :].astype(BF16) for q in range(splits)]
        empty = jnp.zeros((gap, cols), BF16)
        spread = [
            jnp.concatenate(
                [p for q in range(splits) for p in (r[q * cols : (q + 1) * cols], empty)], axis=0
            )
            for r in right
        ]
        none = jnp.zeros((half, gap), BF16)
        wide_left = jnp.concatenate([p for l in left for p in (l, none)], axis=1)
        none = jnp.zeros((splits * LANES, gap), BF16)
        wide_right = jnp.concatenate([p for r in spread for p in (r, none)], axis=1)
        total = dot(wide_left, wide_right, NT)
        for q in range(splits):
            products[q, pl.ds(c, half, owned), :] = total[:, q * LANES : q * LANES + cols]
    for q in range(splits):
        for r in range(near_rows):
            pieces = [products[q, pl.ds((r * rows + i) * owned, owned), :] for i in range(rows)]
            out_ref[q * near_rows + r] = jnp.concatenate(pieces, axis=1).astype(BF16)


def swap(block, distance, members):
    splits, blocks = lax.axis_size("col"), lax.axis_size("row")
    near_rows = members // splits
    pairs = []
    for q in range(splits):
        for r in range(blocks):
            source = q * near_rows + r % near_rows
            to = source ^ distance
            target = (r // near_rows * near_rows + to % near_rows) * splits + to // near_rows
            pairs.append((r * splits + q, target))
    return lax.ppermute(block, ("row", "col"), pairs)


def by_halves(pair_act, tile_mask, w_left_gate, w_left, w_right_gate, w_right, w_out_gate, w_out):
    rows, cols, width = pair_act.shape
    blocks, splits = lax.axis_size("row"), lax.axis_size("col")
    halves = 2
    members = blocks * splits // halves
    near_rows = blocks // halves
    channels = w_left.shape[1]
    owned = channels // members
    pairs = rows * cols
    tile = rows * blocks // TILES
    flat = pair_act.reshape(pairs, width)
    operands = (flat, tile_mask, w_left_gate, w_left, w_right_gate, w_right, w_out_gate)
    left, right, gate = call(
        functools.partial(halves_project_kernel, rows, tile, owned),
        (
            pltpu.VMEM((members, owned, pairs), BF16),
            pltpu.HBM((splits, halves, near_rows, owned, pairs), BF16),
            pltpu.VMEM((pairs, width), F32),
        ),
        operands,
        scratch=[pltpu.VMEM(a.shape, a.dtype) for a in operands]
        + [
            pltpu.VMEM((splits, near_rows, owned, pairs), BF16),
            pltpu.VMEM((pairs, width), BF16),
            pltpu.SemaphoreType.DMA((len(operands),)),
            pltpu.SemaphoreType.DMA((halves,)),
        ],
        flops=10 * pairs * width * channels,
        space=pltpu.HBM,
    )
    right = lax.all_to_all(
        right.reshape(blocks * splits, owned, pairs), ("col", "row"), 0, 0, tiled=True
    )
    held = {0: {d: left[d] for d in range(members)}}
    core, y, z, x = 1, 2, 4, near_rows
    for n, stage in enumerate(((z,), (x, y, x | y), (core,))):
        arrived = {}
        bits = functools.reduce(lambda a, b: a | b, stage)
        for step in stage:
            sent = [(s, d) for s in held for d in held[s] if d & bits == step]
            got = swap(jnp.stack([held[s][d] for s, d in sent]), step, members)
            for m, (s, d) in enumerate(sent):
                arrived.setdefault(s | step, {})[d & ~bits] = got[m]
            if n == 2:
                last, last_steps = got, [s | step for s, d in sent]
        kept = {s: {d: b for d, b in held[s].items() if d & bits == 0} for s in held}
        if n == 2:
            first_steps = sorted(kept)
            first = jnp.stack([kept[s][0] for s in first_steps])
        for s in arrived:
            kept.setdefault(s, {}).update(arrived[s])
        held = kept
    residues = rows * blocks
    triangle = call(
        functools.partial(halves_triangle_kernel, rows, cols, members, (first_steps, last_steps)),
        pltpu.VMEM((members, owned, pairs), BF16),
        (first, last, right.reshape(splits, blocks, owned, pairs)),
        scratch=(
            pltpu.VMEM((splits, near_rows * rows * owned, cols), F32),
            pltpu.VMEM((splits, residues * owned, cols), F32),
            pltpu.VMEM((splits, near_rows * rows * owned, cols), F32),
        ),
        flops=2 * owned * residues**3,
    )
    groups = [
        [q * blocks + h * near_rows + r for q in range(splits) for r in range(near_rows)]
        for h in range(halves)
    ]
    owned_pairs = lax.all_to_all(
        triangle, ("col", "row"), 0, 0, tiled=True, axis_index_groups=groups
    )
    out = call(
        output_kernel,
        jax.ShapeDtypeStruct((pairs, width), BF16),
        (owned_pairs, gate, w_out),
        flops=2 * pairs * width * channels,
    )
    return out.reshape(rows, cols, width)


def by_rows(pair_act, tile_mask, w_left_gate, w_left, w_right_gate, w_right, w_out_gate, w_out):
    rows, cols, _ = pair_act.shape
    normed = norm_axis(pair_act.astype(F32), 2).astype(BF16)
    pair_mask = mask_of(tile_mask, rows, cols)

    def project(weight):
        return jnp.einsum("ijd,de->eij", normed, weight, preferred_element_type=F32)

    left = (jax.nn.sigmoid(project(w_left_gate)) * project(w_left) * pair_mask[None]).astype(BF16)
    right = (jax.nn.sigmoid(project(w_right_gate)) * project(w_right) * pair_mask[None]).astype(
        BF16
    )
    left_rows, right_rows = (
        lax.all_to_all(left, "row", split_axis=0, concat_axis=1, tiled=True),
        lax.all_to_all(right, "row", split_axis=0, concat_axis=1, tiled=True),
    )
    right_block = lax.all_to_all(right_rows, "col", split_axis=1, concat_axis=2, tiled=True)
    triangle = jnp.einsum(
        "cik,cjk->jci",
        lax.all_gather(left_rows, "col", axis=2, tiled=True),
        right_block,
        preferred_element_type=F32,
    )
    triangle = triangle.astype(BF16)
    owned = lax.all_to_all(triangle, "row", split_axis=2, concat_axis=1, tiled=True)
    scaled = norm_axis(owned.astype(F32), 1).astype(BF16)
    projected = jnp.einsum("jci,ce->ije", scaled, w_out, preferred_element_type=F32)
    gate = jax.nn.sigmoid(jnp.einsum("ijd,de->ije", normed, w_out_gate, preferred_element_type=F32))
    return (gate * projected).astype(BF16)


def local(pair_act, tile_mask, w_left_gate, *weights):
    devices = lax.axis_size("row") * lax.axis_size("col")
    rows, cols, _ = pair_act.shape
    channels = w_left_gate.shape[1]
    whole = channels % devices == 0 and 2 * channels // devices % SUBLANES == 0
    aligned = rows * cols % LANES == 0 and cols % SUBLANES == 0 and cols <= LANES
    form = by_channels if whole and aligned else by_rows
    if whole and aligned and lax.axis_size("row") == 16 and lax.axis_size("col") == 2:
        form = by_halves
    return form(pair_act, tile_mask, w_left_gate, *weights)


def solution(mesh):
    return jax.shard_map(
        local,
        mesh=mesh,
        in_specs=(P("row", "col", None), P(), P(), P(), P(), P(), P(), P()),
        out_specs=P("row", "col", None),
        check_vma=False,
    )
```

```python
import functools

import jax
import jax.numpy as jnp
from jax import lax
from jax.experimental import pallas as pl
from jax.experimental.pallas import tpu as pltpu
from jax.sharding import PartitionSpec as P


TILES = 12
LANES = 128
WIDE = 256
OWIDE = 256
SUBLANES = 8
EPS = 1e-05
GRANT = 16 * 2**20
F32 = jnp.float32
BF16 = jnp.bfloat16
NT = (((1,), (1,)), ((), ()))
TN = (((0,), (0,)), ((), ()))


def norm_axis(values, axis):
    mean = jnp.mean(values, axis=axis, keepdims=True)
    centred = values - mean
    spread = jnp.mean(centred * centred, axis=axis, keepdims=True)
    return centred * lax.rsqrt(spread + EPS)


def dot(a, b, dims=(((1,), (0,)), ((), ()))):
    return lax.dot_general(a, b, dims, preferred_element_type=F32)


def lane_mask(cols, tile, pairs, rows, tiles):
    kinds = tiles.shape[0]
    place = lax.broadcasted_iota(jnp.int32, (kinds, pairs), 1).astype(F32) + 0.5
    kind = lax.broadcasted_iota(jnp.int32, (kinds, pairs), 0).astype(F32)
    row = jnp.floor(place * (1.0 / cols))
    col = place - row * cols
    first_row = (lax.axis_index("row") * rows).astype(F32)
    first_col = (lax.axis_index("col") * cols).astype(F32)
    row_kind = jnp.floor((row + first_row + 0.5) * (1.0 / tile))
    col_kind = jnp.floor((col + first_col) * (1.0 / tile))
    row_hot = jnp.where(row_kind == kind, 1.0, 0.0)
    col_hot = jnp.where(col_kind == kind, 1.0, 0.0).astype(BF16)
    return jnp.sum(row_hot * dot(tiles.astype(F32).astype(BF16), col_hot), axis=0, keepdims=True)


def project_kernel(rows, tile, owned, *refs):
    far, (out_ref, gate_ref), near, sems = refs[:7], refs[7:9], refs[9:16], refs[16]
    copies = [pltpu.make_async_copy(a, b, sems.at[n]) for n, (a, b) in enumerate(zip(far, near))]
    for copy in copies:
        copy.start()
    x_ref, tiles_ref, lg_ref, l_ref, rg_ref, r_ref, og_ref = near
    pairs, _ = x_ref.shape
    channels = l_ref.shape[1]
    row = lax.broadcasted_iota(jnp.int32, (2 * channels, channels), 0)
    channel = lax.broadcasted_iota(jnp.int32, (2 * channels, channels), 1)
    within = row % (2 * owned)
    source = row // (2 * owned) * owned + within % owned
    hit = source == channel
    pick_left = jnp.where(hit & (within < owned), 1.0, 0.0).astype(BF16)
    pick_right = jnp.where(hit & (within >= owned), 1.0, 0.0).astype(BF16)
    for copy in copies:
        copy.wait()
    gates = (dot(pick_left, lg_ref[...], NT) + dot(pick_right, rg_ref[...], NT)).astype(BF16)
    values = (dot(pick_left, l_ref[...], NT) + dot(pick_right, r_ref[...], NT)).astype(BF16)
    mask = lane_mask(pairs // rows, tile, pairs, rows, tiles_ref[...]).astype(BF16)
    for start in range(0, pairs, WIDE):
        wide = min(WIDE, pairs - start)
        here = pl.ds(start, wide)
        normed = norm_axis(x_ref[here, :].astype(F32), 1).astype(BF16)
        gate = jax.nn.sigmoid(dot(gates, normed, NT))
        value = dot(values, normed, NT)
        made = (gate * value).astype(BF16) * mask[:, start : start + wide]
        out_ref[:, :, here] = made.reshape(out_ref.shape[0], 2 * owned, wide)
        gate_ref[here, :] = jax.nn.sigmoid(dot(normed, og_ref[...]))


def triangle_kernel(rows, cols, owned, in_ref, out_ref, factors, products):
    splits, blocks = in_ref.shape[0], in_ref.shape[1]
    group = 2 * owned
    for q in range(splits):
        for r in range(blocks):
            flat = in_ref[q, r].astype(F32)
            for i in range(rows):
                at = (r * rows + i) * group
                factors[q, pl.ds(at, group), :] = flat[:, i * cols : (i + 1) * cols]
    residues = blocks * rows
    gap = LANES - cols
    for c in range(owned):
        left = [factors[q, pl.ds(c, residues, group), :].astype(BF16) for q in range(splits)]
        right = [factors[q, pl.ds(owned + c, residues, group), :].astype(BF16) for q in range(splits)]
        empty = jnp.zeros((gap, cols), BF16)
        spread = [
            jnp.concatenate(
                [p for q in range(splits) for p in (r[q * cols : (q + 1) * cols], empty)], axis=0
            )
            for r in right
        ]
        none = jnp.zeros((residues, gap), BF16)
        lefts = jnp.concatenate([p for l in left for p in (l, none)], axis=1)
        none = jnp.zeros((splits * LANES, gap), BF16)
        rights = jnp.concatenate([p for r in spread for p in (r, none)], axis=1)
        total = dot(lefts, rights, NT)
        for q in range(splits):
            products[q, pl.ds(c, residues, owned), :] = total[:, q * LANES : q * LANES + cols]
    for q in range(splits):
        for r in range(blocks):
            pieces = [products[q, pl.ds((r * rows + i) * owned, owned), :] for i in range(rows)]
            out_ref[q, r] = jnp.concatenate(pieces, axis=1).astype(BF16)


def output_kernel(t_ref, gate_ref, w_ref, out_ref):
    pairs = gate_ref.shape[0]
    channels = w_ref.shape[0]
    for start in range(0, pairs, OWIDE):
        wide = min(OWIDE, pairs - start)
        triangle = t_ref[:, :, pl.ds(start, wide)].reshape(channels, wide).astype(F32)
        scaled = norm_axis(triangle, 0).astype(BF16)
        projected = dot(scaled, w_ref[...], TN)
        here = pl.ds(start, wide)
        out_ref[here, :] = (gate_ref[here, :] * projected).astype(BF16)


def space_of(out):
    return getattr(out, "memory_space", pltpu.VMEM)


def call(body, out, operands, scratch=(), flops=0, space=pltpu.VMEM):
    return pl.pallas_call(
        body,
        out_shape=out,
        in_specs=[pl.BlockSpec(memory_space=space)] * len(operands),
        out_specs=jax.tree.map(lambda o: pl.BlockSpec(memory_space=space_of(o)), out),
        scratch_shapes=list(scratch),
        cost_estimate=pl.CostEstimate(flops=flops, bytes_accessed=flops // 100, transcendentals=0),
        compiler_params=pltpu.CompilerParams(vmem_limit_bytes=GRANT),
    )(*[pltpu.with_memory_space_constraint(a, space) for a in operands])


def mask_of(tile_mask, rows, cols):
    tile = rows * lax.axis_size("row") // TILES
    tile_range = lax.iota(jnp.int32, TILES)
    row_ids = (lax.axis_index("row") * rows + lax.iota(jnp.int32, rows)) // tile
    col_ids = (lax.axis_index("col") * cols + lax.iota(jnp.int32, cols)) // tile
    row_hot = (row_ids[:, None] == tile_range[None, :]).astype(F32)
    col_hot = (col_ids[:, None] == tile_range[None, :]).astype(F32)
    some = dot(row_hot, tile_mask.astype(F32))
    return dot(some, col_hot.T)


def by_channels(pair_act, tile_mask, w_left_gate, w_left, w_right_gate, w_right, w_out_gate, w_out):
    rows, cols, width = pair_act.shape
    blocks, splits = lax.axis_size("row"), lax.axis_size("col")
    devices = blocks * splits
    channels = w_left.shape[1]
    owned = channels // devices
    pairs = rows * cols
    tile = rows * blocks // TILES
    flat = pair_act.reshape(pairs, width)
    operands = (flat, tile_mask, w_left_gate, w_left, w_right_gate, w_right, w_out_gate)
    factors, gate = call(
        functools.partial(project_kernel, rows, tile, owned),
        (pltpu.VMEM((devices, 2 * owned, pairs), BF16), pltpu.VMEM((pairs, width), F32)),
        operands,
        scratch=[pltpu.VMEM(a.shape, a.dtype) for a in operands]
        + [pltpu.SemaphoreType.DMA((len(operands),))],
        flops=10 * pairs * width * channels,
        space=pltpu.HBM,
    )
    factors = lax.all_to_all(factors, ("col", "row"), 0, 0, tiled=True)
    residues = rows * blocks
    triangle = call(
        functools.partial(triangle_kernel, rows, cols, owned),
        pltpu.VMEM((splits, blocks, owned, pairs), BF16),
        (factors.reshape(splits, blocks, 2 * owned, pairs),),
        scratch=(
            pltpu.VMEM((splits, residues * 2 * owned, cols), F32),
            pltpu.VMEM((splits, residues * owned, cols), F32),
        ),
        flops=2 * owned * residues**3,
    )
    owned_pairs = lax.all_to_all(
        triangle.reshape(devices, owned, pairs), ("col", "row"), 0, 0, tiled=True
    )
    out = call(
        output_kernel,
        jax.ShapeDtypeStruct((pairs, width), BF16),
        (owned_pairs, gate, w_out),
        flops=2 * pairs * width * channels,
    )
    return out.reshape(rows, cols, width)


def pick_slots(channels, owned, far_bit, value):
    members = channels // owned
    row = lax.broadcasted_iota(jnp.int32, (channels // 2, channels), 0)
    channel = lax.broadcasted_iota(jnp.int32, (channels // 2, channels), 1)
    slot = row // owned
    distance = slot // far_bit * (2 * far_bit) + slot % far_bit + value * far_bit
    owner = distance ^ member_number(members)
    return jnp.where(owner * owned + row % owned == channel, 1.0, 0.0).astype(BF16)


def factor_maker(pick, gate_w, value_w, mask, target):
    gates = dot(pick, gate_w[...], NT).astype(BF16)
    values = dot(pick, value_w[...], NT).astype(BF16)

    def make(normed, start, wide):
        gate = jax.nn.sigmoid(dot(gates, normed, NT))
        made = (gate * dot(values, normed, NT)).astype(BF16) * mask[:, start : start + wide]
        target[..., pl.ds(start, wide)] = made.reshape(*target.shape[:-1], wide)

    return make


def strips_of(pairs):
    return [(start, min(WIDE, pairs - start)) for start in range(0, pairs, WIDE)]


def halves_project_kernel(rows, tile, owned, far_bit, *refs):
    far, (left_ref, right_far, normed_ref), near = refs[:6], refs[6:9], refs[9:15]
    right_ref, sems, right_sems = refs[15:]
    copies = [pltpu.make_async_copy(a, b, sems.at[n]) for n, (a, b) in enumerate(zip(far, near))]
    for copy in copies:
        copy.start()
    x_ref, tiles_ref, lg_ref, l_ref, rg_ref, r_ref = near
    pairs, _ = x_ref.shape
    channels = l_ref.shape[1]
    pick_left = pick_slots(channels, owned, far_bit, 1)
    row = lax.broadcasted_iota(jnp.int32, (channels, channels), 0)
    channel = lax.broadcasted_iota(jnp.int32, (channels, channels), 1)
    pick_right = jnp.where(row == channel, 1.0, 0.0).astype(BF16)
    for copy in copies:
        copy.wait()
    mask = lane_mask(pairs // rows, tile, pairs, rows, tiles_ref[...]).astype(BF16)
    halves = right_far.shape[1]
    make_right = factor_maker(pick_right, rg_ref, r_ref, mask, right_ref)
    make_left = factor_maker(pick_left, lg_ref, l_ref, mask, left_ref)
    for start, wide in strips_of(pairs):
        here = pl.ds(start, wide)
        normed = norm_axis(x_ref[here, :].astype(F32), 1).astype(BF16)
        normed_ref[here, :] = normed
        make_right(normed, start, wide)
    sent = [
        pltpu.make_async_copy(right_ref, right_far.at[:, half], right_sems.at[half])
        for half in range(halves)
    ]
    for copy in sent:
        copy.start()
    for start, wide in strips_of(pairs):
        make_left(normed_ref[pl.ds(start, wide), :], start, wide)
    for copy in sent:
        copy.wait()


def beside_kernel(rows, tile, owned, far_bit, *refs):
    normed_ref, tiles_ref, lg_ref, l_ref, og_ref, left_ref, gate_ref = refs
    pairs = normed_ref.shape[0]
    pick = pick_slots(l_ref.shape[1], owned, far_bit, 0)
    mask = lane_mask(pairs // rows, tile, pairs, rows, tiles_ref[...]).astype(BF16)
    make_left = factor_maker(pick, lg_ref, l_ref, mask, left_ref)
    for start, wide in strips_of(pairs):
        normed = normed_ref[pl.ds(start, wide), :]
        make_left(normed, start, wide)
        gate_ref[pl.ds(start, wide), :] = jax.nn.sigmoid(dot(normed, og_ref[...]))


def layout_kernel(rows, cols, members, splits, steps, *refs):
    left_refs, (out_ref, lefts) = refs[: len(steps)], refs[len(steps) :]
    owned, half = out_ref.shape[:2]
    near_rows = members // splits
    me = member_number(members)
    for left_ref, distances in zip(left_refs, steps):
        for n, distance in enumerate(distances):
            source = me ^ distance
            q, r = source // near_rows, source % near_rows
            flat = left_ref[n].astype(F32)
            for i in range(rows):
                at = pl.multiple_of((r * rows + i) * owned, owned)
                lefts[q, pl.ds(at, owned), :] = flat[:, i * cols : (i + 1) * cols]
    none = jnp.zeros((half, LANES - cols), BF16)
    for c in range(owned):
        parts = [lefts[q, pl.ds(c, half, owned), :].astype(BF16) for q in range(splits)]
        out_ref[c] = jnp.concatenate([p for part in parts for p in (part, none)], axis=1)


def member_number(members):
    near_rows = members // lax.axis_size("col")
    return lax.axis_index("col") * near_rows + lax.axis_index("row") % near_rows


def halves_triangle_kernel(rows, cols, members, left_ref, right_ref, out_ref, rights, products):
    splits, blocks, owned = right_ref.shape[:3]
    near_rows = members // splits
    for q in range(splits):
        for r in range(blocks):
            flat = right_ref[q, r].astype(F32)
            for i in range(rows):
                at = (r * rows + i) * owned
                rights[q, pl.ds(at, owned), :] = flat[:, i * cols : (i + 1) * cols]
    residues, half = blocks * rows, near_rows * rows
    gap = LANES - cols
    for c in range(owned):
        right = [rights[q, pl.ds(c, residues, owned), :].astype(BF16) for q in range(splits)]
        empty = jnp.zeros((gap, cols), BF16)
        spread = [
            jnp.concatenate(
                [p for q in range(splits) for p in (r[q * cols : (q + 1) * cols], empty)], axis=0
            )
            for r in right
        ]
        none = jnp.zeros((splits * LANES, gap), BF16)
        wide_right = jnp.concatenate([p for r in spread for p in (r, none)], axis=1)
        total = dot(left_ref[c], wide_right, NT)
        for q in range(splits):
            products[q, pl.ds(c, half, owned), :] = total[:, q * LANES : q * LANES + cols]
    for q in range(splits):
        for r in range(near_rows):
            pieces = [products[q, pl.ds((r * rows + i) * owned, owned), :] for i in range(rows)]
            out_ref[q * near_rows + r] = jnp.concatenate(pieces, axis=1).astype(BF16)


def swap(block, distance, members):
    splits, blocks = lax.axis_size("col"), lax.axis_size("row")
    near_rows = members // splits
    pairs = []
    for q in range(splits):
        for r in range(blocks):
            source = q * near_rows + r % near_rows
            to = source ^ distance
            target = (r // near_rows * near_rows + to % near_rows) * splits + to // near_rows
            pairs.append((r * splits + q, target))
    return lax.ppermute(block, ("row", "col"), pairs)


def by_halves(pair_act, tile_mask, w_left_gate, w_left, w_right_gate, w_right, w_out_gate, w_out):
    rows, cols, width = pair_act.shape
    blocks, splits = lax.axis_size("row"), lax.axis_size("col")
    halves = 2
    members = blocks * splits // halves
    near_rows = blocks // halves
    channels = w_left.shape[1]
    owned = channels // members
    pairs = rows * cols
    tile = rows * blocks // TILES
    flat = pair_act.reshape(pairs, width)
    core, y, z, x = 1, 2, 4, near_rows
    operands = (flat, tile_mask, w_left_gate, w_left, w_right_gate, w_right)
    left, right, normed = call(
        functools.partial(halves_project_kernel, rows, tile, owned, z),
        (
            pltpu.VMEM((members // 2, owned, pairs), BF16),
            pltpu.HBM((splits, halves, near_rows, owned, pairs), BF16),
            pltpu.VMEM((pairs, width), BF16),
        ),
        operands,
        scratch=[pltpu.VMEM(a.shape, a.dtype) for a in operands]
        + [
            pltpu.VMEM((splits, near_rows, owned, pairs), BF16),
            pltpu.SemaphoreType.DMA((len(operands),)),
            pltpu.SemaphoreType.DMA((halves,)),
        ],
        flops=8 * pairs * width * channels,
        space=pltpu.HBM,
    )
    right = lax.all_to_all(
        right.reshape(blocks * splits, owned, pairs), ("col", "row"), 0, 0, tiled=True
    )
    got = swap(left, z, members)
    stayed, gate = call(
        functools.partial(beside_kernel, rows, tile, owned, z),
        (
            pltpu.VMEM((members // 2, owned, pairs), BF16),
            pltpu.VMEM((pairs, width), F32),
        ),
        (normed, tile_mask, w_left_gate, w_left, w_out_gate),
        flops=6 * pairs * width * channels,
    )
    near = [d for d in range(members) if not d & z]
    held = {0: dict(zip(near, stayed)), z: dict(zip(near, got))}
    for stage in ((x, y, x | y), (core,)):
        arrived, kept = {}, {}
        bits = functools.reduce(lambda a, b: a | b, stage)
        for step in stage:
            sent = [(s, d) for s in held for d in held[s] if d & bits == step]
            got = swap(jnp.stack([held[s][d] for s, d in sent]), step, members)
            last_steps = [s | step for s, d in sent]
            for m, (s, d) in enumerate(sent):
                arrived.setdefault(s | step, {})[d & ~bits] = got[m]
        for s in held:
            kept[s] = {d: b for d, b in held[s].items() if d & bits == 0}
        first_steps, first = sorted(kept), [kept[s][0] for s in sorted(kept)]
        held = {**kept, **arrived}
    left = call(
        functools.partial(layout_kernel, rows, cols, members, splits, (first_steps, last_steps)),
        pltpu.VMEM((owned, near_rows * rows, splits * LANES), BF16),
        (jnp.stack(first), got),
        scratch=[pltpu.VMEM((splits, near_rows * rows * owned, cols), F32)],
        flops=pairs * channels * 10,
    )
    residues = rows * blocks
    triangle = call(
        functools.partial(halves_triangle_kernel, rows, cols, members),
        pltpu.VMEM((members, owned, pairs), BF16),
        (left, right.reshape(splits, blocks, owned, pairs)),
        scratch=(
            pltpu.VMEM((splits, residues * owned, cols), F32),
            pltpu.VMEM((splits, near_rows * rows * owned, cols), F32),
        ),
        flops=2 * owned * residues**3,
    )
    groups = [
        [q * blocks + h * near_rows + r for q in range(splits) for r in range(near_rows)]
        for h in range(halves)
    ]
    owned_pairs = lax.all_to_all(
        triangle, ("col", "row"), 0, 0, tiled=True, axis_index_groups=groups
    )
    out = call(
        output_kernel,
        jax.ShapeDtypeStruct((pairs, width), BF16),
        (owned_pairs, gate, w_out),
        flops=2 * pairs * width * channels,
    )
    return out.reshape(rows, cols, width)


def by_rows(pair_act, tile_mask, w_left_gate, w_left, w_right_gate, w_right, w_out_gate, w_out):
    rows, cols, _ = pair_act.shape
    normed = norm_axis(pair_act.astype(F32), 2).astype(BF16)
    pair_mask = mask_of(tile_mask, rows, cols)

    def project(weight):
        return jnp.einsum("ijd,de->eij", normed, weight, preferred_element_type=F32)

    left = (jax.nn.sigmoid(project(w_left_gate)) * project(w_left) * pair_mask[None]).astype(BF16)
    right = (jax.nn.sigmoid(project(w_right_gate)) * project(w_right) * pair_mask[None]).astype(
        BF16
    )
    left_rows, right_rows = (
        lax.all_to_all(left, "row", split_axis=0, concat_axis=1, tiled=True),
        lax.all_to_all(right, "row", split_axis=0, concat_axis=1, tiled=True),
    )
    right_block = lax.all_to_all(right_rows, "col", split_axis=1, concat_axis=2, tiled=True)
    triangle = jnp.einsum(
        "cik,cjk->jci",
        lax.all_gather(left_rows, "col", axis=2, tiled=True),
        right_block,
        preferred_element_type=F32,
    )
    triangle = triangle.astype(BF16)
    owned = lax.all_to_all(triangle, "row", split_axis=2, concat_axis=1, tiled=True)
    scaled = norm_axis(owned.astype(F32), 1).astype(BF16)
    projected = jnp.einsum("jci,ce->ije", scaled, w_out, preferred_element_type=F32)
    gate = jax.nn.sigmoid(jnp.einsum("ijd,de->ije", normed, w_out_gate, preferred_element_type=F32))
    return (gate * projected).astype(BF16)


def local(pair_act, tile_mask, w_left_gate, *weights):
    devices = lax.axis_size("row") * lax.axis_size("col")
    rows, cols, _ = pair_act.shape
    channels = w_left_gate.shape[1]
    whole = channels % devices == 0 and 2 * channels // devices % SUBLANES == 0
    aligned = rows * cols % LANES == 0 and cols % SUBLANES == 0 and cols <= LANES
    form = by_channels if whole and aligned else by_rows
    if whole and aligned and lax.axis_size("row") == 16 and lax.axis_size("col") == 2:
        form = by_halves
    return form(pair_act, tile_mask, w_left_gate, *weights)


def solution(mesh):
    return jax.shard_map(
        local,
        mesh=mesh,
        in_specs=(P("row", "col", None), P(), P(), P(), P(), P(), P(), P()),
        out_specs=P("row", "col", None),
        check_vma=False,
    )
```

```python
import functools

import jax
import jax.numpy as jnp
from jax import lax
from jax.experimental import pallas as pl
from jax.experimental.pallas import tpu as pltpu
from jax.sharding import PartitionSpec as P


TILES = 12
LANES = 128
WIDE = 256
OWIDE = 256
SUBLANES = 8
EPS = 1e-05
GRANT = 16 * 2**20
F32 = jnp.float32
BF16 = jnp.bfloat16
NT = (((1,), (1,)), ((), ()))
TN = (((0,), (0,)), ((), ()))


def norm_axis(values, axis):
    mean = jnp.mean(values, axis=axis, keepdims=True)
    centred = values - mean
    spread = jnp.mean(centred * centred, axis=axis, keepdims=True)
    return centred * lax.rsqrt(spread + EPS)


def dot(a, b, dims=(((1,), (0,)), ((), ()))):
    return lax.dot_general(a, b, dims, preferred_element_type=F32)


def gather_strip(ref, start, wide, cols):
    gap = LANES - cols
    tail = ref.shape[0] // LANES * cols
    parts = []
    for group in range(start // LANES, (start + wide) // LANES):
        parts.append(ref[pl.ds(group * cols, cols), :])
        parts.append(ref[pl.ds(tail + group * gap, gap), :])
    return jnp.concatenate(parts, axis=0)


def scatter_strip(ref, start, wide, cols, values):
    gap = LANES - cols
    tail = ref.shape[0] // LANES * cols
    for n, group in enumerate(range(start // LANES, (start + wide) // LANES)):
        at = n * LANES
        ref[pl.ds(group * cols, cols), :] = values[at : at + cols]
        ref[pl.ds(tail + group * gap, gap), :] = values[at + cols : at + LANES]


def rows_of(flat, rows, cols):
    groups = flat.shape[1] // LANES
    gap = LANES - cols
    pieces = [flat[:, g * LANES : g * LANES + cols] for g in range(groups)]
    ends = [flat[:, g * LANES + cols : (g + 1) * LANES] for g in range(groups)]
    each = cols // gap
    for n in range(rows - groups):
        pieces.append(jnp.concatenate(ends[n * each : (n + 1) * each], axis=1))
    return pieces


def flat_of(pieces, cols):
    gap = LANES - cols
    each = cols // gap
    groups = len(pieces) * cols // LANES
    parts = []
    for g in range(groups):
        end = pieces[groups + g // each]
        parts += [pieces[g], end[:, g % each * gap : (g % each + 1) * gap]]
    return jnp.concatenate(parts, axis=1)


def lane_mask(cols, tile, pairs, rows, tiles):
    kinds = tiles.shape[0]
    lane = lax.broadcasted_iota(jnp.int32, (kinds, pairs), 1)
    gap = LANES - cols
    tail = pairs // LANES * cols - cols
    within = lane % LANES
    group = lane // LANES
    flat = jnp.where(within < cols, group * cols + within, tail + group * gap + within)
    place = flat.astype(F32) + 0.5
    kind = lax.broadcasted_iota(jnp.int32, (kinds, pairs), 0).astype(F32)
    row = jnp.floor(place * (1.0 / cols))
    col = place - row * cols
    first_row = (lax.axis_index("row") * rows).astype(F32)
    first_col = (lax.axis_index("col") * cols).astype(F32)
    row_kind = jnp.floor((row + first_row + 0.5) * (1.0 / tile))
    col_kind = jnp.floor((col + first_col) * (1.0 / tile))
    row_hot = jnp.where(row_kind == kind, 1.0, 0.0)
    col_hot = jnp.where(col_kind == kind, 1.0, 0.0).astype(BF16)
    return jnp.sum(row_hot * dot(tiles.astype(F32).astype(BF16), col_hot), axis=0, keepdims=True)


def output_kernel(cols, places, t_ref, gate_ref, w_ref, out_ref):
    pairs = gate_ref.shape[0]
    for start in range(0, pairs, OWIDE):
        wide = min(OWIDE, pairs - start)
        here = pl.ds(start, wide)
        triangle = jnp.concatenate([t_ref[p, :, here].astype(F32) for p in places], axis=0)
        scaled = norm_axis(triangle, 0).astype(BF16)
        projected = dot(scaled, w_ref[...], TN)
        here = pl.ds(start, wide)
        scatter_strip(out_ref, start, wide, cols, (gate_ref[here, :] * projected).astype(BF16))


def space_of(out):
    return getattr(out, "memory_space", pltpu.VMEM)


def call(body, out, operands, scratch=(), flops=0, space=pltpu.VMEM):
    return pl.pallas_call(
        body,
        out_shape=out,
        in_specs=[pl.BlockSpec(memory_space=space)] * len(operands),
        out_specs=jax.tree.map(lambda o: pl.BlockSpec(memory_space=space_of(o)), out),
        scratch_shapes=list(scratch),
        cost_estimate=pl.CostEstimate(flops=flops, bytes_accessed=flops // 100, transcendentals=0),
        compiler_params=pltpu.CompilerParams(vmem_limit_bytes=GRANT),
    )(*[pltpu.with_memory_space_constraint(a, space) for a in operands])


def mask_of(tile_mask, rows, cols):
    tile = rows * lax.axis_size("row") // TILES
    tile_range = lax.iota(jnp.int32, TILES)
    row_ids = (lax.axis_index("row") * rows + lax.iota(jnp.int32, rows)) // tile
    col_ids = (lax.axis_index("col") * cols + lax.iota(jnp.int32, cols)) // tile
    row_hot = (row_ids[:, None] == tile_range[None, :]).astype(F32)
    col_hot = (col_ids[:, None] == tile_range[None, :]).astype(F32)
    some = dot(row_hot, tile_mask.astype(F32))
    return dot(some, col_hot.T)


def pick_slots(channels, owned, far_bit, value):
    members = channels // owned
    row = lax.broadcasted_iota(jnp.int32, (channels // 2, channels), 0)
    channel = lax.broadcasted_iota(jnp.int32, (channels // 2, channels), 1)
    slot = row // owned
    distance = slot // far_bit * (2 * far_bit) + slot % far_bit + value * far_bit
    owner = distance ^ member_number(members)
    return jnp.where(owner * owned + row % owned == channel, 1.0, 0.0).astype(BF16)


def factor_maker(pick, gate_w, value_w, mask, target):
    gates = dot(pick, gate_w[...], NT).astype(BF16)
    values = dot(pick, value_w[...], NT).astype(BF16)

    def make(normed, start, wide):
        gate = jax.nn.sigmoid(dot(gates, normed, NT))
        made = (gate * dot(values, normed, NT)).astype(BF16) * mask[:, start : start + wide]
        target[..., pl.ds(start, wide)] = made.reshape(*target.shape[:-1], wide)

    return make


def strips_of(pairs):
    return [(start, min(WIDE, pairs - start)) for start in range(0, pairs, WIDE)]


def halves_project_kernel(rows, tile, owned, far_bit, *refs):
    far, (left_ref, right_far, normed_ref), near = refs[:6], refs[6:9], refs[9:15]
    right_ref, sems, right_sems = refs[15:]
    copies = [pltpu.make_async_copy(a, b, sems.at[n]) for n, (a, b) in enumerate(zip(far, near))]
    for copy in copies:
        copy.start()
    x_ref, tiles_ref, lg_ref, l_ref, rg_ref, r_ref = near
    pairs, _ = x_ref.shape
    channels = l_ref.shape[1]
    pick_left = pick_slots(channels, owned, far_bit, 1)
    row = lax.broadcasted_iota(jnp.int32, (channels, channels), 0)
    channel = lax.broadcasted_iota(jnp.int32, (channels, channels), 1)
    pick_right = jnp.where(row == channel, 1.0, 0.0).astype(BF16)
    for copy in copies:
        copy.wait()
    mask = lane_mask(pairs // rows, tile, pairs, rows, tiles_ref[...]).astype(BF16)
    halves = right_far.shape[1]
    make_right = factor_maker(pick_right, rg_ref, r_ref, mask, right_ref)
    make_left = factor_maker(pick_left, lg_ref, l_ref, mask, left_ref)
    for start, wide in strips_of(pairs):
        here = pl.ds(start, wide)
        strip = gather_strip(x_ref, start, wide, pairs // rows)
        normed = norm_axis(strip.astype(F32), 1).astype(BF16)
        normed_ref[here, :] = normed
        make_right(normed, start, wide)
    splits = right_far.shape[0]
    sent = [
        pltpu.make_async_copy(right_ref.at[q], right_far.at[q, half], right_sems.at[q, half])
        for q in range(splits)
        for half in range(halves)
    ]
    for copy in sent:
        copy.start()
    for start, wide in strips_of(pairs):
        make_left(normed_ref[pl.ds(start, wide), :], start, wide)
    for copy in sent:
        copy.wait()


def beside_kernel(rows, tile, owned, far_bit, *refs):
    normed_ref, tiles_ref, lg_ref, l_ref, og_ref, left_ref, gate_ref = refs
    pairs = normed_ref.shape[0]
    pick = pick_slots(l_ref.shape[1], owned, far_bit, 0)
    mask = lane_mask(pairs // rows, tile, pairs, rows, tiles_ref[...]).astype(BF16)
    make_left = factor_maker(pick, lg_ref, l_ref, mask, left_ref)
    for start, wide in strips_of(pairs):
        normed = normed_ref[pl.ds(start, wide), :]
        make_left(normed, start, wide)
        gate_ref[pl.ds(start, wide), :] = jax.nn.sigmoid(dot(normed, og_ref[...]))


def layout_kernel(rows, cols, members, splits, steps, *refs):
    left_refs, (out_ref, lefts) = refs[: len(steps)], refs[len(steps) :]
    owned, half = out_ref.shape[:2]
    near_rows = members // splits
    me = member_number(members)
    for left_ref, distances in zip(left_refs, steps):
        for n, distance in enumerate(distances):
            source = me ^ distance
            q, r = source // near_rows, source % near_rows
            for i, piece in enumerate(rows_of(left_ref[n].astype(F32), rows, cols)):
                at = pl.multiple_of((r * rows + i) * owned, owned)
                lefts[q, pl.ds(at, owned), :] = piece
    none = jnp.zeros((half, LANES - cols), BF16)
    for c in range(owned):
        parts = [lefts[q, pl.ds(c, half, owned), :].astype(BF16) for q in range(splits)]
        out_ref[c] = jnp.concatenate([p for part in parts for p in (part, none)], axis=1)


def member_number(members):
    near_rows = members // lax.axis_size("col")
    return lax.axis_index("col") * near_rows + lax.axis_index("row") % near_rows


def halves_triangle_kernel(rows, cols, members, left_ref, right_ref, out_ref, rights, products):
    splits, blocks, owned = right_ref.shape[:3]
    near_rows = members // splits
    for q in range(splits):
        for r in range(blocks):
            for i, piece in enumerate(rows_of(right_ref[q, r].astype(F32), rows, cols)):
                rights[q, pl.ds((r * rows + i) * owned, owned), :] = piece
    residues, half = blocks * rows, near_rows * rows
    gap = LANES - cols
    for c in range(owned):
        right = [rights[q, pl.ds(c, residues, owned), :].astype(BF16) for q in range(splits)]
        empty = jnp.zeros((gap, cols), BF16)
        spread = [
            jnp.concatenate(
                [p for q in range(splits) for p in (r[q * cols : (q + 1) * cols], empty)], axis=0
            )
            for r in right
        ]
        none = jnp.zeros((splits * LANES, gap), BF16)
        wide_right = jnp.concatenate([p for r in spread for p in (r, none)], axis=1)
        total = dot(left_ref[c], wide_right, NT)
        for q in range(splits):
            products[q, pl.ds(c, half, owned), :] = total[:, q * LANES : q * LANES + cols]
    for q in range(splits):
        for r in range(near_rows):
            pieces = [products[q, pl.ds((r * rows + i) * owned, owned), :] for i in range(rows)]
            out_ref[place_of(q * near_rows + r, near_rows)] = flat_of(pieces, cols).astype(BF16)


def place_of(member, near_rows):
    far_bit = near_rows // 2
    row = member % near_rows
    return member - row + row % far_bit * 2 + row // far_bit


def swap(block, distance, members):
    splits, blocks = lax.axis_size("col"), lax.axis_size("row")
    near_rows = members // splits
    pairs = []
    for q in range(splits):
        for r in range(blocks):
            source = q * near_rows + r % near_rows
            to = source ^ distance
            target = (r // near_rows * near_rows + to % near_rows) * splits + to // near_rows
            pairs.append((r * splits + q, target))
    return lax.ppermute(block, ("row", "col"), pairs)


def by_halves(pair_act, tile_mask, w_left_gate, w_left, w_right_gate, w_right, w_out_gate, w_out):
    rows, cols, width = pair_act.shape
    blocks, splits = lax.axis_size("row"), lax.axis_size("col")
    halves = 2
    members = blocks * splits // halves
    near_rows = blocks // halves
    channels = w_left.shape[1]
    owned = channels // members
    pairs = rows * cols
    tile = rows * blocks // TILES
    flat = pair_act.reshape(pairs, width)
    core, y, z, x = 1, 2, 4, near_rows
    operands = (flat, tile_mask, w_left_gate, w_left, w_right_gate, w_right)
    left, right, normed = call(
        functools.partial(halves_project_kernel, rows, tile, owned, z),
        (
            pltpu.VMEM((members // 2, owned, pairs), BF16),
            pltpu.HBM((splits, halves, near_rows, owned, pairs), BF16),
            pltpu.VMEM((pairs, width), BF16),
        ),
        operands,
        scratch=[pltpu.VMEM(a.shape, a.dtype) for a in operands]
        + [
            pltpu.VMEM((splits, near_rows, owned, pairs), BF16),
            pltpu.SemaphoreType.DMA((len(operands),)),
            pltpu.SemaphoreType.DMA((splits, halves)),
        ],
        flops=8 * pairs * width * channels,
        space=pltpu.HBM,
    )
    right = lax.all_to_all(
        right.reshape(blocks * splits, owned, pairs), ("col", "row"), 0, 0, tiled=True
    )
    got = swap(left, z, members)
    stayed, gate = call(
        functools.partial(beside_kernel, rows, tile, owned, z),
        (
            pltpu.VMEM((members // 2, owned, pairs), BF16),
            pltpu.VMEM((pairs, width), F32),
        ),
        (normed, tile_mask, w_left_gate, w_left, w_out_gate),
        flops=6 * pairs * width * channels,
    )
    near = [d for d in range(members) if not d & z]
    held = {0: dict(zip(near, stayed)), z: dict(zip(near, got))}
    for stage in ((x, y, x | y), (core,)):
        arrived, kept = {}, {}
        bits = functools.reduce(lambda a, b: a | b, stage)
        for step in stage:
            sent = [(s, d) for s in held for d in held[s] if d & bits == step]
            got = swap(jnp.stack([held[s][d] for s, d in sent]), step, members)
            last_steps = [s | step for s, d in sent]
            for m, (s, d) in enumerate(sent):
                arrived.setdefault(s | step, {})[d & ~bits] = got[m]
        for s in held:
            kept[s] = {d: b for d, b in held[s].items() if d & bits == 0}
        first_steps, first = sorted(kept), [kept[s][0] for s in sorted(kept)]
        held = {**kept, **arrived}
    left = call(
        functools.partial(layout_kernel, rows, cols, members, splits, (first_steps, last_steps)),
        pltpu.VMEM((owned, near_rows * rows, splits * LANES), BF16),
        (jnp.stack(first), got),
        scratch=[pltpu.VMEM((splits, near_rows * rows * owned, cols), F32)],
        flops=pairs * channels * 10,
    )
    residues = rows * blocks
    triangle = call(
        functools.partial(halves_triangle_kernel, rows, cols, members),
        pltpu.VMEM((members, owned, pairs), BF16),
        (left, right.reshape(splits, blocks, owned, pairs)),
        scratch=(
            pltpu.VMEM((splits, residues * owned, cols), F32),
            pltpu.VMEM((splits, near_rows * rows * owned, cols), F32),
        ),
        flops=2 * owned * residues**3,
    )
    order = sorted(range(members), key=lambda m: place_of(m, near_rows))
    groups = [
        [m // near_rows * blocks + h * near_rows + m % near_rows for m in order]
        for h in range(halves)
    ]
    owned_pairs = lax.all_to_all(
        triangle, ("col", "row"), 0, 0, tiled=True, axis_index_groups=groups
    )
    out = call(
        functools.partial(output_kernel, cols, [place_of(m, near_rows) for m in range(members)]),
        jax.ShapeDtypeStruct((pairs, width), BF16),
        (owned_pairs, gate, w_out),
        flops=2 * pairs * width * channels,
    )
    return out.reshape(rows, cols, width)


def by_rows(pair_act, tile_mask, w_left_gate, w_left, w_right_gate, w_right, w_out_gate, w_out):
    rows, cols, _ = pair_act.shape
    normed = norm_axis(pair_act.astype(F32), 2).astype(BF16)
    pair_mask = mask_of(tile_mask, rows, cols)

    def project(weight):
        return jnp.einsum("ijd,de->eij", normed, weight, preferred_element_type=F32)

    left = (jax.nn.sigmoid(project(w_left_gate)) * project(w_left) * pair_mask[None]).astype(BF16)
    right = (jax.nn.sigmoid(project(w_right_gate)) * project(w_right) * pair_mask[None]).astype(
        BF16
    )
    left_rows, right_rows = (
        lax.all_to_all(left, "row", split_axis=0, concat_axis=1, tiled=True),
        lax.all_to_all(right, "row", split_axis=0, concat_axis=1, tiled=True),
    )
    right_block = lax.all_to_all(right_rows, "col", split_axis=1, concat_axis=2, tiled=True)
    triangle = jnp.einsum(
        "cik,cjk->jci",
        lax.all_gather(left_rows, "col", axis=2, tiled=True),
        right_block,
        preferred_element_type=F32,
    )
    triangle = triangle.astype(BF16)
    owned = lax.all_to_all(triangle, "row", split_axis=2, concat_axis=1, tiled=True)
    scaled = norm_axis(owned.astype(F32), 1).astype(BF16)
    projected = jnp.einsum("jci,ce->ije", scaled, w_out, preferred_element_type=F32)
    gate = jax.nn.sigmoid(jnp.einsum("ijd,de->ije", normed, w_out_gate, preferred_element_type=F32))
    return (gate * projected).astype(BF16)


def local(pair_act, tile_mask, w_left_gate, *weights):
    blocks, splits = lax.axis_size("row"), lax.axis_size("col")
    rows, cols, _ = pair_act.shape
    channels = w_left_gate.shape[1]
    halved = blocks == 2 * 2**3 and splits == 2 and channels * 2 == blocks * splits * SUBLANES
    aligned = rows * cols % LANES == 0 and cols < LANES and cols % (LANES - cols) == 0
    packed = (LANES - cols) % (2 * SUBLANES) == 0 and cols % (2 * SUBLANES) == 0
    form = by_halves if halved and aligned and packed else by_rows
    return form(pair_act, tile_mask, w_left_gate, *weights)


def solution(mesh):
    return jax.shard_map(
        local,
        mesh=mesh,
        in_specs=(P("row", "col", None), P(), P(), P(), P(), P(), P(), P()),
        out_specs=P("row", "col", None),
        check_vma=False,
    )
```

```python
import functools

import jax
import jax.numpy as jnp
from jax import lax
from jax.experimental import pallas as pl
from jax.experimental.pallas import tpu as pltpu
from jax.sharding import PartitionSpec as P


TILES = 12
LANES = 128
WIDE = 256
OWIDE = 256
SUBLANES = 8
EPS = 1e-05
GRANT = 16 * 2**20
F32 = jnp.float32
BF16 = jnp.bfloat16
NT = (((1,), (1,)), ((), ()))
TN = (((0,), (0,)), ((), ()))


def norm_axis(values, axis):
    mean = jnp.mean(values, axis=axis, keepdims=True)
    centred = values - mean
    spread = jnp.mean(centred * centred, axis=axis, keepdims=True)
    return centred * lax.rsqrt(spread + EPS)


def dot(a, b, dims=(((1,), (0,)), ((), ()))):
    return lax.dot_general(a, b, dims, preferred_element_type=F32)


def gather_strip(ref, start, wide, cols):
    gap = LANES - cols
    tail = ref.shape[0] // LANES * cols
    parts = []
    for group in range(start // LANES, (start + wide) // LANES):
        parts.append(ref[pl.ds(group * cols, cols), :])
        parts.append(ref[pl.ds(tail + group * gap, gap), :])
    return jnp.concatenate(parts, axis=0)


def scatter_strip(ref, start, wide, cols, values):
    gap = LANES - cols
    tail = ref.shape[0] // LANES * cols
    for n, group in enumerate(range(start // LANES, (start + wide) // LANES)):
        at = n * LANES
        ref[pl.ds(group * cols, cols), :] = values[at : at + cols]
        ref[pl.ds(tail + group * gap, gap), :] = values[at + cols : at + LANES]


def rows_of(flat, rows, cols):
    groups = flat.shape[1] // LANES
    gap = LANES - cols
    pieces = [flat[:, g * LANES : g * LANES + cols] for g in range(groups)]
    ends = [flat[:, g * LANES + cols : (g + 1) * LANES] for g in range(groups)]
    each = cols // gap
    for n in range(rows - groups):
        pieces.append(jnp.concatenate(ends[n * each : (n + 1) * each], axis=1))
    return pieces


def flat_of(pieces, cols):
    gap = LANES - cols
    each = cols // gap
    groups = len(pieces) * cols // LANES
    parts = []
    for g in range(groups):
        end = pieces[groups + g // each]
        parts += [pieces[g], end[:, g % each * gap : (g % each + 1) * gap]]
    return jnp.concatenate(parts, axis=1)


def lane_mask(cols, tile, pairs, rows, tiles):
    kinds = tiles.shape[0]
    lane = lax.broadcasted_iota(jnp.int32, (kinds, pairs), 1)
    gap = LANES - cols
    tail = pairs // LANES * cols - cols
    within = lane % LANES
    group = lane // LANES
    flat = jnp.where(within < cols, group * cols + within, tail + group * gap + within)
    place = flat.astype(F32) + 0.5
    kind = lax.broadcasted_iota(jnp.int32, (kinds, pairs), 0).astype(F32)
    row = jnp.floor(place * (1.0 / cols))
    col = place - row * cols
    first_row = (lax.axis_index("row") * rows).astype(F32)
    first_col = (lax.axis_index("col") * cols).astype(F32)
    row_kind = jnp.floor((row + first_row + 0.5) * (1.0 / tile))
    col_kind = jnp.floor((col + first_col) * (1.0 / tile))
    row_hot = jnp.where(row_kind == kind, 1.0, 0.0)
    col_hot = jnp.where(col_kind == kind, 1.0, 0.0).astype(BF16)
    return jnp.sum(row_hot * dot(tiles.astype(F32).astype(BF16), col_hot), axis=0, keepdims=True)


def output_kernel(cols, places, t_ref, gate_ref, w_ref, out_ref):
    pairs = gate_ref.shape[0]
    for start in range(0, pairs, OWIDE):
        wide = min(OWIDE, pairs - start)
        here = pl.ds(start, wide)
        triangle = jnp.concatenate([t_ref[p, :, here].astype(F32) for p in places], axis=0)
        scaled = norm_axis(triangle, 0).astype(BF16)
        projected = dot(scaled, w_ref[...], TN)
        here = pl.ds(start, wide)
        scatter_strip(out_ref, start, wide, cols, (gate_ref[here, :] * projected).astype(BF16))


def space_of(out):
    return getattr(out, "memory_space", pltpu.VMEM)


def call(body, out, operands, scratch=(), flops=0, space=pltpu.VMEM):
    return pl.pallas_call(
        body,
        out_shape=out,
        in_specs=[pl.BlockSpec(memory_space=space)] * len(operands),
        out_specs=jax.tree.map(lambda o: pl.BlockSpec(memory_space=space_of(o)), out),
        scratch_shapes=list(scratch),
        cost_estimate=pl.CostEstimate(flops=flops, bytes_accessed=flops // 100, transcendentals=0),
        compiler_params=pltpu.CompilerParams(vmem_limit_bytes=GRANT),
    )(*[pltpu.with_memory_space_constraint(a, space) for a in operands])


def mask_of(tile_mask, rows, cols):
    tile = rows * lax.axis_size("row") // TILES
    tile_range = lax.iota(jnp.int32, TILES)
    row_ids = (lax.axis_index("row") * rows + lax.iota(jnp.int32, rows)) // tile
    col_ids = (lax.axis_index("col") * cols + lax.iota(jnp.int32, cols)) // tile
    row_hot = (row_ids[:, None] == tile_range[None, :]).astype(F32)
    col_hot = (col_ids[:, None] == tile_range[None, :]).astype(F32)
    some = dot(row_hot, tile_mask.astype(F32))
    return dot(some, col_hot.T)


def pick_slots(channels, owned, far_bit, value):
    members = channels // owned
    row = lax.broadcasted_iota(jnp.int32, (channels // 2, channels), 0)
    channel = lax.broadcasted_iota(jnp.int32, (channels // 2, channels), 1)
    slot = row // owned
    distance = slot // far_bit * (2 * far_bit) + slot % far_bit + value * far_bit
    owner = distance ^ member_number(members)
    return jnp.where(owner * owned + row % owned == channel, 1.0, 0.0).astype(BF16)


def factor_maker(pick, gate_w, value_w, mask, target):
    gates = dot(pick, gate_w[...], NT).astype(BF16)
    values = dot(pick, value_w[...], NT).astype(BF16)

    def make(normed, start, wide):
        gate = jax.nn.sigmoid(dot(gates, normed, NT))
        made = (gate * dot(values, normed, NT)).astype(BF16) * mask[:, start : start + wide]
        target[..., pl.ds(start, wide)] = made.reshape(*target.shape[:-1], wide)

    return make


def strips_of(pairs):
    return [(start, min(WIDE, pairs - start)) for start in range(0, pairs, WIDE)]


def halves_project_kernel(rows, tile, owned, far_bit, *refs):
    far, (left_ref, right_far, normed_ref), near = refs[:6], refs[6:9], refs[9:15]
    right_ref, sems, right_sems = refs[15:]
    copies = [pltpu.make_async_copy(a, b, sems.at[n]) for n, (a, b) in enumerate(zip(far, near))]
    for copy in copies:
        copy.start()
    x_ref, tiles_ref, lg_ref, l_ref, rg_ref, r_ref = near
    pairs, _ = x_ref.shape
    channels = l_ref.shape[1]
    pick_left = pick_slots(channels, owned, far_bit, 1)
    row = lax.broadcasted_iota(jnp.int32, (channels, channels), 0)
    channel = lax.broadcasted_iota(jnp.int32, (channels, channels), 1)
    splits, far_rows = right_ref.shape[0], right_ref.shape[2]
    near_rows = right_ref.shape[1] * far_rows
    slot = row // owned
    member = slot // near_rows * near_rows + slot % far_rows * far_bit + slot % near_rows // far_rows
    pick_right = jnp.where(member * owned + row % owned == channel, 1.0, 0.0).astype(BF16)
    for copy in copies:
        copy.wait()
    mask = lane_mask(pairs // rows, tile, pairs, rows, tiles_ref[...]).astype(BF16)
    halves = right_far.shape[2]
    make_right = factor_maker(pick_right, rg_ref, r_ref, mask, right_ref)
    make_left = factor_maker(pick_left, lg_ref, l_ref, mask, left_ref)
    for start, wide in strips_of(pairs):
        here = pl.ds(start, wide)
        strip = gather_strip(x_ref, start, wide, pairs // rows)
        normed = norm_axis(strip.astype(F32), 1).astype(BF16)
        normed_ref[here, :] = normed
        make_right(normed, start, wide)
    sent = [
        pltpu.make_async_copy(right_ref.at[q], right_far.at[q, :, half], right_sems.at[q, half])
        for q in range(splits)
        for half in range(halves)
    ]
    for copy in sent:
        copy.start()
    for start, wide in strips_of(pairs):
        make_left(normed_ref[pl.ds(start, wide), :], start, wide)
    for copy in sent:
        copy.wait()


def beside_kernel(rows, tile, owned, far_bit, *refs):
    normed_ref, tiles_ref, lg_ref, l_ref, og_ref, left_ref, gate_ref = refs
    pairs = normed_ref.shape[0]
    pick = pick_slots(l_ref.shape[1], owned, far_bit, 0)
    mask = lane_mask(pairs // rows, tile, pairs, rows, tiles_ref[...]).astype(BF16)
    make_left = factor_maker(pick, lg_ref, l_ref, mask, left_ref)
    for start, wide in strips_of(pairs):
        normed = normed_ref[pl.ds(start, wide), :]
        make_left(normed, start, wide)
        gate_ref[pl.ds(start, wide), :] = jax.nn.sigmoid(dot(normed, og_ref[...]))


def layout_kernel(rows, cols, members, splits, steps, *refs):
    left_refs, (out_ref, lefts) = refs[: len(steps)], refs[len(steps) :]
    owned, half = out_ref.shape[:2]
    near_rows = members // splits
    me = member_number(members)
    for left_ref, distances in zip(left_refs, steps):
        for n, distance in enumerate(distances):
            source = me ^ distance
            q, r = source // near_rows, source % near_rows
            for i, piece in enumerate(rows_of(left_ref[n].astype(F32), rows, cols)):
                at = pl.multiple_of((r * rows + i) * owned, owned)
                lefts[q, pl.ds(at, owned), :] = piece
    none = jnp.zeros((half, LANES - cols), BF16)
    for c in range(owned):
        parts = [lefts[q, pl.ds(c, half, owned), :].astype(BF16) for q in range(splits)]
        out_ref[c] = jnp.concatenate([p for part in parts for p in (part, none)], axis=1)


def member_number(members):
    near_rows = members // lax.axis_size("col")
    return lax.axis_index("col") * near_rows + lax.axis_index("row") % near_rows


def halves_triangle_kernel(rows, cols, members, lines, left_ref, right_ref, out_ref, rights, products):
    splits, blocks, owned = right_ref.shape[:3]
    near_rows = members // splits
    for q in range(splits):
        for n, r in enumerate(lines):
            for i, piece in enumerate(rows_of(right_ref[q, n].astype(F32), rows, cols)):
                rights[q, pl.ds((r * rows + i) * owned, owned), :] = piece
    residues, half = blocks * rows, near_rows * rows
    gap = LANES - cols
    for c in range(owned):
        right = [rights[q, pl.ds(c, residues, owned), :].astype(BF16) for q in range(splits)]
        empty = jnp.zeros((gap, cols), BF16)
        spread = [
            jnp.concatenate(
                [p for q in range(splits) for p in (r[q * cols : (q + 1) * cols], empty)], axis=0
            )
            for r in right
        ]
        none = jnp.zeros((splits * LANES, gap), BF16)
        wide_right = jnp.concatenate([p for r in spread for p in (r, none)], axis=1)
        total = dot(left_ref[c], wide_right, NT)
        for q in range(splits):
            products[q, pl.ds(c, half, owned), :] = total[:, q * LANES : q * LANES + cols]
    for q in range(splits):
        for r in range(near_rows):
            pieces = [products[q, pl.ds((r * rows + i) * owned, owned), :] for i in range(rows)]
            out_ref[place_of(q * near_rows + r, near_rows)] = flat_of(pieces, cols).astype(BF16)


def place_of(member, near_rows):
    far_bit = near_rows // 2
    row = member % near_rows
    return member - row + row % far_bit * 2 + row // far_bit


def swap(block, distance, members):
    splits, blocks = lax.axis_size("col"), lax.axis_size("row")
    near_rows = members // splits
    pairs = []
    for q in range(splits):
        for r in range(blocks):
            source = q * near_rows + r % near_rows
            to = source ^ distance
            target = (r // near_rows * near_rows + to % near_rows) * splits + to // near_rows
            pairs.append((r * splits + q, target))
    return lax.ppermute(block, ("row", "col"), pairs)


def by_halves(pair_act, tile_mask, w_left_gate, w_left, w_right_gate, w_right, w_out_gate, w_out):
    rows, cols, width = pair_act.shape
    blocks, splits = lax.axis_size("row"), lax.axis_size("col")
    halves = 2
    members = blocks * splits // halves
    near_rows = blocks // halves
    channels = w_left.shape[1]
    owned = channels // members
    pairs = rows * cols
    tile = rows * blocks // TILES
    flat = pair_act.reshape(pairs, width)
    core, y, z, x = 1, 2, 4, near_rows
    operands = (flat, tile_mask, w_left_gate, w_left, w_right_gate, w_right)
    left, right, normed = call(
        functools.partial(halves_project_kernel, rows, tile, owned, z),
        (
            pltpu.VMEM((members // 2, owned, pairs), BF16),
            pltpu.HBM((splits, z, halves, near_rows // z, owned, pairs), BF16),
            pltpu.VMEM((pairs, width), BF16),
        ),
        operands,
        scratch=[pltpu.VMEM(a.shape, a.dtype) for a in operands]
        + [
            pltpu.VMEM((splits, z, near_rows // z, owned, pairs), BF16),
            pltpu.SemaphoreType.DMA((len(operands),)),
            pltpu.SemaphoreType.DMA((splits, halves)),
        ],
        flops=8 * pairs * width * channels,
        space=pltpu.HBM,
    )
    lines = sorted(range(blocks), key=lambda r: (r % z, r // z))
    everyone = [[q * blocks + r for q in range(splits) for r in lines]]
    right = lax.all_to_all(
        right.reshape(blocks * splits, owned, pairs),
        ("col", "row"),
        0,
        0,
        tiled=True,
        axis_index_groups=everyone,
    )
    got = swap(left, z, members)
    stayed, gate = call(
        functools.partial(beside_kernel, rows, tile, owned, z),
        (
            pltpu.VMEM((members // 2, owned, pairs), BF16),
            pltpu.VMEM((pairs, width), F32),
        ),
        (normed, tile_mask, w_left_gate, w_left, w_out_gate),
        flops=6 * pairs * width * channels,
    )
    near = [d for d in range(members) if not d & z]
    held = {0: dict(zip(near, stayed)), z: dict(zip(near, got))}
    for stage in ((x, y, x | y), (core,)):
        arrived, kept = {}, {}
        bits = functools.reduce(lambda a, b: a | b, stage)
        for step in stage:
            sent = [(s, d) for s in held for d in held[s] if d & bits == step]
            got = swap(jnp.stack([held[s][d] for s, d in sent]), step, members)
            last_steps = [s | step for s, d in sent]
            for m, (s, d) in enumerate(sent):
                arrived.setdefault(s | step, {})[d & ~bits] = got[m]
        for s in held:
            kept[s] = {d: b for d, b in held[s].items() if d & bits == 0}
        first_steps, first = sorted(kept), [kept[s][0] for s in sorted(kept)]
        held = {**kept, **arrived}
    left = call(
        functools.partial(layout_kernel, rows, cols, members, splits, (first_steps, last_steps)),
        pltpu.VMEM((owned, near_rows * rows, splits * LANES), BF16),
        (jnp.stack(first), got),
        scratch=[pltpu.VMEM((splits, near_rows * rows * owned, cols), F32)],
        flops=pairs * channels * 10,
    )
    residues = rows * blocks
    triangle = call(
        functools.partial(halves_triangle_kernel, rows, cols, members, lines),
        pltpu.VMEM((members, owned, pairs), BF16),
        (left, right.reshape(splits, blocks, owned, pairs)),
        scratch=(
            pltpu.VMEM((splits, residues * owned, cols), F32),
            pltpu.VMEM((splits, near_rows * rows * owned, cols), F32),
        ),
        flops=2 * owned * residues**3,
    )
    order = sorted(range(members), key=lambda m: place_of(m, near_rows))
    groups = [
        [m // near_rows * blocks + h * near_rows + m % near_rows for m in order]
        for h in range(halves)
    ]
    owned_pairs = lax.all_to_all(
        triangle, ("col", "row"), 0, 0, tiled=True, axis_index_groups=groups
    )
    out = call(
        functools.partial(output_kernel, cols, [place_of(m, near_rows) for m in range(members)]),
        jax.ShapeDtypeStruct((pairs, width), BF16),
        (owned_pairs, gate, w_out),
        flops=2 * pairs * width * channels,
    )
    return out.reshape(rows, cols, width)


def by_rows(pair_act, tile_mask, w_left_gate, w_left, w_right_gate, w_right, w_out_gate, w_out):
    rows, cols, _ = pair_act.shape
    normed = norm_axis(pair_act.astype(F32), 2).astype(BF16)
    pair_mask = mask_of(tile_mask, rows, cols)

    def project(weight):
        return jnp.einsum("ijd,de->eij", normed, weight, preferred_element_type=F32)

    left = (jax.nn.sigmoid(project(w_left_gate)) * project(w_left) * pair_mask[None]).astype(BF16)
    right = (jax.nn.sigmoid(project(w_right_gate)) * project(w_right) * pair_mask[None]).astype(
        BF16
    )
    left_rows, right_rows = (
        lax.all_to_all(left, "row", split_axis=0, concat_axis=1, tiled=True),
        lax.all_to_all(right, "row", split_axis=0, concat_axis=1, tiled=True),
    )
    right_block = lax.all_to_all(right_rows, "col", split_axis=1, concat_axis=2, tiled=True)
    triangle = jnp.einsum(
        "cik,cjk->jci",
        lax.all_gather(left_rows, "col", axis=2, tiled=True),
        right_block,
        preferred_element_type=F32,
    )
    triangle = triangle.astype(BF16)
    owned = lax.all_to_all(triangle, "row", split_axis=2, concat_axis=1, tiled=True)
    scaled = norm_axis(owned.astype(F32), 1).astype(BF16)
    projected = jnp.einsum("jci,ce->ije", scaled, w_out, preferred_element_type=F32)
    gate = jax.nn.sigmoid(jnp.einsum("ijd,de->ije", normed, w_out_gate, preferred_element_type=F32))
    return (gate * projected).astype(BF16)


def local(pair_act, tile_mask, w_left_gate, *weights):
    blocks, splits = lax.axis_size("row"), lax.axis_size("col")
    rows, cols, _ = pair_act.shape
    channels = w_left_gate.shape[1]
    halved = blocks == 2 * 2**3 and splits == 2 and channels * 2 == blocks * splits * SUBLANES
    aligned = rows * cols % LANES == 0 and cols < LANES and cols % (LANES - cols) == 0
    packed = (LANES - cols) % (2 * SUBLANES) == 0 and cols % (2 * SUBLANES) == 0
    form = by_halves if halved and aligned and packed else by_rows
    return form(pair_act, tile_mask, w_left_gate, *weights)


def solution(mesh):
    return jax.shard_map(
        local,
        mesh=mesh,
        in_specs=(P("row", "col", None), P(), P(), P(), P(), P(), P(), P()),
        out_specs=P("row", "col", None),
        check_vma=False,
    )
```

```python
import functools

import jax
import jax.numpy as jnp
from jax import lax
from jax.experimental import pallas as pl
from jax.experimental.pallas import tpu as pltpu
from jax.sharding import PartitionSpec as P


TILES = 12
LANES = 128
WIDE = 1152
OWIDE = 256
SUBLANES = 8
EPS = 1e-05
GRANT = 16 * 2**20
F32 = jnp.float32
BF16 = jnp.bfloat16
NT = (((1,), (1,)), ((), ()))
TN = (((0,), (0,)), ((), ()))


def norm_axis(values, axis):
    mean = jnp.mean(values, axis=axis, keepdims=True)
    centred = values - mean
    spread = jnp.mean(centred * centred, axis=axis, keepdims=True)
    return centred * lax.rsqrt(spread + EPS)


def dot(a, b, dims=(((1,), (0,)), ((), ()))):
    return lax.dot_general(a, b, dims, preferred_element_type=F32)


def gather_strip(ref, start, wide, cols):
    gap = LANES - cols
    tail = ref.shape[0] // LANES * cols
    parts = []
    for group in range(start // LANES, (start + wide) // LANES):
        parts.append(ref[pl.ds(group * cols, cols), :])
        parts.append(ref[pl.ds(tail + group * gap, gap), :])
    return jnp.concatenate(parts, axis=0)


def scatter_strip(ref, start, wide, cols, values):
    gap = LANES - cols
    tail = ref.shape[0] // LANES * cols
    for n, group in enumerate(range(start // LANES, (start + wide) // LANES)):
        at = n * LANES
        ref[pl.ds(group * cols, cols), :] = values[at : at + cols]
        ref[pl.ds(tail + group * gap, gap), :] = values[at + cols : at + LANES]


def rows_of(flat, rows, cols):
    groups = flat.shape[1] // LANES
    gap = LANES - cols
    pieces = [flat[:, g * LANES : g * LANES + cols] for g in range(groups)]
    ends = [flat[:, g * LANES + cols : (g + 1) * LANES] for g in range(groups)]
    each = cols // gap
    for n in range(rows - groups):
        pieces.append(jnp.concatenate(ends[n * each : (n + 1) * each], axis=1))
    return pieces


def flat_of(pieces, cols):
    gap = LANES - cols
    each = cols // gap
    groups = len(pieces) * cols // LANES
    parts = []
    for g in range(groups):
        end = pieces[groups + g // each]
        parts += [pieces[g], end[:, g % each * gap : (g % each + 1) * gap]]
    return jnp.concatenate(parts, axis=1)


def lane_hots(cols, tile, pairs, rows, kinds):
    lane = lax.broadcasted_iota(jnp.int32, (kinds, pairs), 1)
    gap = LANES - cols
    tail = pairs // LANES * cols - cols
    within = lane % LANES
    group = lane // LANES
    flat = jnp.where(within < cols, group * cols + within, tail + group * gap + within)
    place = flat.astype(F32) + 0.5
    kind = lax.broadcasted_iota(jnp.int32, (kinds, pairs), 0).astype(F32)
    row = jnp.floor(place * (1.0 / cols))
    col = place - row * cols
    first_row = (lax.axis_index("row") * rows).astype(F32)
    first_col = (lax.axis_index("col") * cols).astype(F32)
    row_kind = jnp.floor((row + first_row + 0.5) * (1.0 / tile))
    col_kind = jnp.floor((col + first_col) * (1.0 / tile))
    row_hot = jnp.where(row_kind == kind, 1.0, 0.0)
    col_hot = jnp.where(col_kind == kind, 1.0, 0.0).astype(BF16)
    return row_hot, col_hot


def lane_mask(hots, tiles):
    row_hot, col_hot = hots
    return jnp.sum(row_hot * dot(tiles.astype(F32).astype(BF16), col_hot), axis=0, keepdims=True)


def output_kernel(cols, places, t_ref, gate_ref, w_ref, out_ref):
    pairs = gate_ref.shape[0]
    for start in range(0, pairs, OWIDE):
        wide = min(OWIDE, pairs - start)
        here = pl.ds(start, wide)
        triangle = jnp.concatenate([t_ref[p, :, here].astype(F32) for p in places], axis=0)
        scaled = norm_axis(triangle, 0).astype(BF16)
        projected = dot(scaled, w_ref[...], TN)
        here = pl.ds(start, wide)
        scatter_strip(out_ref, start, wide, cols, (gate_ref[here, :] * projected).astype(BF16))


def space_of(out):
    return getattr(out, "memory_space", pltpu.VMEM)


def call(body, out, operands, scratch=(), flops=0, space=pltpu.VMEM):
    return pl.pallas_call(
        body,
        out_shape=out,
        in_specs=[pl.BlockSpec(memory_space=space)] * len(operands),
        out_specs=jax.tree.map(lambda o: pl.BlockSpec(memory_space=space_of(o)), out),
        scratch_shapes=list(scratch),
        cost_estimate=pl.CostEstimate(flops=flops, bytes_accessed=flops // 100, transcendentals=0),
        compiler_params=pltpu.CompilerParams(vmem_limit_bytes=GRANT),
    )(*[pltpu.with_memory_space_constraint(a, space) for a in operands])


def mask_of(tile_mask, rows, cols):
    tile = rows * lax.axis_size("row") // TILES
    tile_range = lax.iota(jnp.int32, TILES)
    row_ids = (lax.axis_index("row") * rows + lax.iota(jnp.int32, rows)) // tile
    col_ids = (lax.axis_index("col") * cols + lax.iota(jnp.int32, cols)) // tile
    row_hot = (row_ids[:, None] == tile_range[None, :]).astype(F32)
    col_hot = (col_ids[:, None] == tile_range[None, :]).astype(F32)
    some = dot(row_hot, tile_mask.astype(F32))
    return dot(some, col_hot.T)


def pick_slots(channels, owned, far_bit, value):
    members = channels // owned
    row = lax.broadcasted_iota(jnp.int32, (channels // 2, channels), 0)
    channel = lax.broadcasted_iota(jnp.int32, (channels // 2, channels), 1)
    slot = row // owned
    distance = slot // far_bit * (2 * far_bit) + slot % far_bit + value * far_bit
    owner = distance ^ member_number(members)
    return jnp.where(owner * owned + row % owned == channel, 1.0, 0.0).astype(BF16)


def factor_maker(pick, gate_w, value_w, mask, target):
    gates = dot(pick, gate_w[...], NT).astype(BF16)
    values = dot(pick, value_w[...], NT).astype(BF16)

    def make(normed, start, wide):
        gate = jax.nn.sigmoid(dot(gates, normed, NT))
        made = (gate * dot(values, normed, NT)).astype(BF16) * mask[:, start : start + wide]
        target[..., pl.ds(start, wide)] = made.reshape(*target.shape[:-1], wide)

    return make


def strips_of(pairs):
    return [(start, min(WIDE, pairs - start)) for start in range(0, pairs, WIDE)]


def halves_project_kernel(rows, tile, owned, far_bit, *refs):
    far, (left_ref, right_far, normed_ref), near = refs[:6], refs[6:9], refs[9:15]
    right_ref, sems, right_sems = refs[15:]
    copies = [pltpu.make_async_copy(a, b, sems.at[n]) for n, (a, b) in enumerate(zip(far, near))]
    for copy in copies:
        copy.start()
    x_ref, tiles_ref, lg_ref, l_ref, rg_ref, r_ref = near
    pairs, _ = x_ref.shape
    channels = l_ref.shape[1]
    pick_left = pick_slots(channels, owned, far_bit, 1)
    row = lax.broadcasted_iota(jnp.int32, (channels, channels), 0)
    channel = lax.broadcasted_iota(jnp.int32, (channels, channels), 1)
    splits, far_rows = right_ref.shape[0], right_ref.shape[2]
    near_rows = right_ref.shape[1] * far_rows
    slot = row // owned
    member = slot // near_rows * near_rows + slot % far_rows * far_bit + slot % near_rows // far_rows
    pick_right = jnp.where(member * owned + row % owned == channel, 1.0, 0.0).astype(BF16)
    hots = lane_hots(pairs // rows, tile, pairs, rows, tiles_ref.shape[0])
    for copy in copies[:2] + copies[4:]:
        copy.wait()
    mask = lane_mask(hots, tiles_ref[...]).astype(BF16)
    halves = right_far.shape[2]
    make_right = factor_maker(pick_right, rg_ref, r_ref, mask, right_ref)
    for start, wide in strips_of(pairs):
        here = pl.ds(start, wide)
        strip = gather_strip(x_ref, start, wide, pairs // rows)
        normed = norm_axis(strip.astype(F32), 1).astype(BF16)
        normed_ref[here, :] = normed
        make_right(normed, start, wide)
    sent = [
        pltpu.make_async_copy(right_ref.at[q], right_far.at[q, :, half], right_sems.at[q, half])
        for q in range(splits)
        for half in range(halves)
    ]
    for copy in sent:
        copy.start()
    for copy in copies[2:4]:
        copy.wait()
    make_left = factor_maker(pick_left, lg_ref, l_ref, mask, left_ref)
    for start, wide in strips_of(pairs):
        make_left(normed_ref[pl.ds(start, wide), :], start, wide)
    for copy in sent:
        copy.wait()


def beside_kernel(rows, tile, owned, far_bit, *refs):
    normed_ref, tiles_ref, lg_ref, l_ref, og_ref, left_ref, gate_ref = refs
    pairs = normed_ref.shape[0]
    pick = pick_slots(l_ref.shape[1], owned, far_bit, 0)
    hots = lane_hots(pairs // rows, tile, pairs, rows, tiles_ref.shape[0])
    mask = lane_mask(hots, tiles_ref[...]).astype(BF16)
    make_left = factor_maker(pick, lg_ref, l_ref, mask, left_ref)
    for start, wide in strips_of(pairs):
        normed = normed_ref[pl.ds(start, wide), :]
        make_left(normed, start, wide)
        gate_ref[pl.ds(start, wide), :] = jax.nn.sigmoid(dot(normed, og_ref[...]))


def layout_kernel(rows, cols, members, splits, steps, *refs):
    left_refs, (out_ref, lefts) = refs[: len(steps)], refs[len(steps) :]
    owned, half = out_ref.shape[:2]
    near_rows = members // splits
    me = member_number(members)
    for left_ref, distances in zip(left_refs, steps):
        for n, distance in enumerate(distances):
            source = me ^ distance
            q, r = source // near_rows, source % near_rows
            for i, piece in enumerate(rows_of(left_ref[n].astype(F32), rows, cols)):
                at = pl.multiple_of((r * rows + i) * owned, owned)
                lefts[q, pl.ds(at, owned), :] = piece
    none = jnp.zeros((half, LANES - cols), BF16)
    for c in range(owned):
        parts = [lefts[q, pl.ds(c, half, owned), :].astype(BF16) for q in range(splits)]
        out_ref[c] = jnp.concatenate([p for part in parts for p in (part, none)], axis=1)


def member_number(members):
    near_rows = members // lax.axis_size("col")
    return lax.axis_index("col") * near_rows + lax.axis_index("row") % near_rows


def halves_triangle_kernel(rows, cols, members, lines, left_ref, right_ref, out_ref, rights, products):
    splits, blocks, owned = right_ref.shape[:3]
    near_rows = members // splits
    for q in range(splits):
        for n, r in enumerate(lines):
            for i, piece in enumerate(rows_of(right_ref[q, n].astype(F32), rows, cols)):
                rights[q, pl.ds((r * rows + i) * owned, owned), :] = piece
    residues, half = blocks * rows, near_rows * rows
    gap = LANES - cols
    for c in range(owned):
        right = [rights[q, pl.ds(c, residues, owned), :].astype(BF16) for q in range(splits)]
        empty = jnp.zeros((gap, cols), BF16)
        spread = [
            jnp.concatenate(
                [p for q in range(splits) for p in (r[q * cols : (q + 1) * cols], empty)], axis=0
            )
            for r in right
        ]
        none = jnp.zeros((splits * LANES, gap), BF16)
        wide_right = jnp.concatenate([p for r in spread for p in (r, none)], axis=1)
        total = dot(left_ref[c], wide_right, NT)
        for q in range(splits):
            products[q, pl.ds(c, half, owned), :] = total[:, q * LANES : q * LANES + cols]
    for q in range(splits):
        for r in range(near_rows):
            pieces = [products[q, pl.ds((r * rows + i) * owned, owned), :] for i in range(rows)]
            out_ref[place_of(q * near_rows + r, near_rows)] = flat_of(pieces, cols).astype(BF16)


def place_of(member, near_rows):
    far_bit = near_rows // 2
    row = member % near_rows
    return member - row + row % far_bit * 2 + row // far_bit


def swap(block, distance, members):
    splits, blocks = lax.axis_size("col"), lax.axis_size("row")
    near_rows = members // splits
    pairs = []
    for q in range(splits):
        for r in range(blocks):
            source = q * near_rows + r % near_rows
            to = source ^ distance
            target = (r // near_rows * near_rows + to % near_rows) * splits + to // near_rows
            pairs.append((r * splits + q, target))
    return lax.ppermute(block, ("row", "col"), pairs)


def by_halves(pair_act, tile_mask, w_left_gate, w_left, w_right_gate, w_right, w_out_gate, w_out):
    rows, cols, width = pair_act.shape
    blocks, splits = lax.axis_size("row"), lax.axis_size("col")
    halves = 2
    members = blocks * splits // halves
    near_rows = blocks // halves
    channels = w_left.shape[1]
    owned = channels // members
    pairs = rows * cols
    tile = rows * blocks // TILES
    flat = pair_act.reshape(pairs, width)
    core, y, z, x = 1, 2, 4, near_rows
    operands = (flat, tile_mask, w_left_gate, w_left, w_right_gate, w_right)
    left, right, normed = call(
        functools.partial(halves_project_kernel, rows, tile, owned, z),
        (
            pltpu.VMEM((members // 2, owned, pairs), BF16),
            pltpu.HBM((splits, z, halves, near_rows // z, owned, pairs), BF16),
            pltpu.VMEM((pairs, width), BF16),
        ),
        operands,
        scratch=[pltpu.VMEM(a.shape, a.dtype) for a in operands]
        + [
            pltpu.VMEM((splits, z, near_rows // z, owned, pairs), BF16),
            pltpu.SemaphoreType.DMA((len(operands),)),
            pltpu.SemaphoreType.DMA((splits, halves)),
        ],
        flops=8 * pairs * width * channels,
        space=pltpu.HBM,
    )
    lines = sorted(range(blocks), key=lambda r: (r % z, r // z))
    everyone = [[q * blocks + r for q in range(splits) for r in lines]]
    right = lax.all_to_all(
        right.reshape(blocks * splits, owned, pairs),
        ("col", "row"),
        0,
        0,
        tiled=True,
        axis_index_groups=everyone,
    )
    got = swap(left, z, members)
    stayed, gate = call(
        functools.partial(beside_kernel, rows, tile, owned, z),
        (
            pltpu.VMEM((members // 2, owned, pairs), BF16),
            pltpu.VMEM((pairs, width), F32),
        ),
        (normed, tile_mask, w_left_gate, w_left, w_out_gate),
        flops=6 * pairs * width * channels,
    )
    near = [d for d in range(members) if not d & z]
    held = {0: dict(zip(near, stayed)), z: dict(zip(near, got))}
    for stage in ((x, y, x | y), (core,)):
        arrived, kept = {}, {}
        bits = functools.reduce(lambda a, b: a | b, stage)
        for step in stage:
            sent = [(s, d) for s in held for d in held[s] if d & bits == step]
            got = swap(jnp.stack([held[s][d] for s, d in sent]), step, members)
            last_steps = [s | step for s, d in sent]
            for m, (s, d) in enumerate(sent):
                arrived.setdefault(s | step, {})[d & ~bits] = got[m]
        for s in held:
            kept[s] = {d: b for d, b in held[s].items() if d & bits == 0}
        first_steps, first = sorted(kept), [kept[s][0] for s in sorted(kept)]
        held = {**kept, **arrived}
    left = call(
        functools.partial(layout_kernel, rows, cols, members, splits, (first_steps, last_steps)),
        pltpu.VMEM((owned, near_rows * rows, splits * LANES), BF16),
        (jnp.stack(first), got),
        scratch=[pltpu.VMEM((splits, near_rows * rows * owned, cols), F32)],
        flops=pairs * channels * 10,
    )
    residues = rows * blocks
    triangle = call(
        functools.partial(halves_triangle_kernel, rows, cols, members, lines),
        pltpu.VMEM((members, owned, pairs), BF16),
        (left, right.reshape(splits, blocks, owned, pairs)),
        scratch=(
            pltpu.VMEM((splits, residues * owned, cols), F32),
            pltpu.VMEM((splits, near_rows * rows * owned, cols), F32),
        ),
        flops=2 * owned * residues**3,
    )
    order = sorted(range(members), key=lambda m: place_of(m, near_rows))
    groups = [
        [m // near_rows * blocks + h * near_rows + m % near_rows for m in order]
        for h in range(halves)
    ]
    owned_pairs = lax.all_to_all(
        triangle, ("col", "row"), 0, 0, tiled=True, axis_index_groups=groups
    )
    out = call(
        functools.partial(output_kernel, cols, [place_of(m, near_rows) for m in range(members)]),
        jax.ShapeDtypeStruct((pairs, width), BF16),
        (owned_pairs, gate, w_out),
        flops=2 * pairs * width * channels,
    )
    return out.reshape(rows, cols, width)


def by_rows(pair_act, tile_mask, w_left_gate, w_left, w_right_gate, w_right, w_out_gate, w_out):
    rows, cols, _ = pair_act.shape
    normed = norm_axis(pair_act.astype(F32), 2).astype(BF16)
    pair_mask = mask_of(tile_mask, rows, cols)

    def project(weight):
        return jnp.einsum("ijd,de->eij", normed, weight, preferred_element_type=F32)

    left = (jax.nn.sigmoid(project(w_left_gate)) * project(w_left) * pair_mask[None]).astype(BF16)
    right = (jax.nn.sigmoid(project(w_right_gate)) * project(w_right) * pair_mask[None]).astype(
        BF16
    )
    left_rows, right_rows = (
        lax.all_to_all(left, "row", split_axis=0, concat_axis=1, tiled=True),
        lax.all_to_all(right, "row", split_axis=0, concat_axis=1, tiled=True),
    )
    right_block = lax.all_to_all(right_rows, "col", split_axis=1, concat_axis=2, tiled=True)
    triangle = jnp.einsum(
        "cik,cjk->jci",
        lax.all_gather(left_rows, "col", axis=2, tiled=True),
        right_block,
        preferred_element_type=F32,
    )
    triangle = triangle.astype(BF16)
    owned = lax.all_to_all(triangle, "row", split_axis=2, concat_axis=1, tiled=True)
    scaled = norm_axis(owned.astype(F32), 1).astype(BF16)
    projected = jnp.einsum("jci,ce->ije", scaled, w_out, preferred_element_type=F32)
    gate = jax.nn.sigmoid(jnp.einsum("ijd,de->ije", normed, w_out_gate, preferred_element_type=F32))
    return (gate * projected).astype(BF16)


def local(pair_act, tile_mask, w_left_gate, *weights):
    blocks, splits = lax.axis_size("row"), lax.axis_size("col")
    rows, cols, _ = pair_act.shape
    channels = w_left_gate.shape[1]
    halved = blocks == 2 * 2**3 and splits == 2 and channels * 2 == blocks * splits * SUBLANES
    aligned = rows * cols % LANES == 0 and cols < LANES and cols % (LANES - cols) == 0
    packed = (LANES - cols) % (2 * SUBLANES) == 0 and cols % (2 * SUBLANES) == 0
    form = by_halves if halved and aligned and packed else by_rows
    return form(pair_act, tile_mask, w_left_gate, *weights)


def solution(mesh):
    return jax.shard_map(
        local,
        mesh=mesh,
        in_specs=(P("row", "col", None), P(), P(), P(), P(), P(), P(), P()),
        out_specs=P("row", "col", None),
        check_vma=False,
    )
```
